256 devices in a mesh: groups: 4 (over y, x), tm: 32 (over z), space: 2 (over core).
Axes of the slice: x: 2, y: 2, z: 32, core: 2. Of those that a mesh axis runs over, the one named last changes fastest.
The devices are a block of a 4x8x32 slice.
Arguments:
- query_pre: bfloat16 [128, 8, 32, 2240], P(('groups', 'tm'), 'space'), parts along dimension 0, may hold values from -6 to 6
- key_pre: bfloat16 [128, 8, 32, 2240], P(('groups', 'tm'), 'space'), parts along dimension 0, may hold values from -6 to 6
- value_pre: bfloat16 [128, 8, 32, 2240], P(('groups', 'tm'), 'space'), parts along dimension 0, may hold values from -8 to 8
- grad_out: bfloat16 [128, 8, 32, 2240], P(('groups', 'tm'), 'space'), parts along dimension 0, may hold values from -96 to 96
- conv_taps: float32 [3, 3, 2240], replicated, may hold values from -4 to 4
Outputs:
- attended: bfloat16 [128, 8, 32, 2240], P(('groups', 'tm'), 'space'), parts along dimension 0
- query_grad: bfloat16 [128, 8, 32, 2240], P(('groups', 'tm'), 'space'), parts along dimension 0
- key_grad: bfloat16 [128, 8, 32, 2240], P(('groups', 'tm'), 'space'), parts along dimension 0
- value_grad: bfloat16 [128, 8, 32, 2240], P(('groups', 'tm'), 'space'), parts along dimension 0
- taps_grad: float32 [12, 3, 2240], P('groups'), parts along dimension 0
The draws below stay inside these ranges and needn't reach their ends.
There are 4 independent parts, one for each index of `groups`. The reference program is written for one: setup_inputs(seed, part) draws one part's arguments, and reference() takes and returns one part's arrays. A program takes and returns all parts, laid end to end along the dimension named above; an argument that names none is the same for every part. Nothing has to cross between parts.
All inputs are finite; a program needn't handle non-finite values.
Results may differ from the reference program's by a relative error of at most 0.013.
Values may be sent and summed in bfloat16 or wider, within the bound.
No kernel may reach another device: no remote copies, remote signals or barrier semaphores. Data moves between devices by JAX's collectives and lax.ppermute only.
A program may use at most 128 MiB of HBM per device.

```python
import jax
import jax.numpy as jnp
from jax import lax

HEADS = 20
HEAD_DIM = 112
COLS = 32
D = 2240
FRAMES = 32
ROWS = 8


def draw_value_pre(key, part):
    first, second, third = jax.random.split(jax.random.fold_in(key, 71), 3)
    frame_mean = jax.random.normal(first, (FRAMES, 1, 1, D), jnp.float32)
    row_mean = 0.5 * jax.random.normal(second, (FRAMES, ROWS, 1, D), jnp.float32)
    noise = jax.random.normal(third, (FRAMES, ROWS, COLS, D), jnp.float32)
    drawn = frame_mean + row_mean + noise
    return jnp.clip(drawn, -8.0, 8.0).astype(jnp.bfloat16)


def level_of(rng, extent, cuts, low, high):
    gain, own = 1.0, jax.random.fold_in(rng, 6)
    for position, blocks in cuts:
        draws = jnp.exp(jax.random.uniform(jax.random.fold_in(own, position), (blocks,), jnp.float32, low / len(cuts), high / len(cuts)))
        gain = gain * jnp.repeat(draws, extent[position] // blocks).reshape([-1 if axis == position else 1 for axis in range(len(extent))])
    return gain


def bell_draw(key, dims, width, most, pieces=(), dtype=jnp.bfloat16):
    values = jax.random.normal(key, dims, jnp.float32) * width
    if len(pieces) > 0:
        values = level_of(key, dims, pieces, -0.22, 0.18) * values
    return jnp.clip(values, min=-most, max=most).astype(dtype)


def setup_inputs(seed: int = 0, part: int = 0) -> dict:
    splits = jax.random.split(jax.random.key(seed), 6)
    part_keys = jax.random.split(jax.random.fold_in(splits[5], part), 6)
    return {
        "query_pre": bell_draw(part_keys[0], (FRAMES, ROWS, COLS, D), 1.0, 6.0, ((0, 32), (1, 2))),
        "key_pre": bell_draw(part_keys[1], (FRAMES, ROWS, COLS, D), 1.0, 6.0, ((0, 32), (1, 2))),
        "value_pre": draw_value_pre(jax.random.fold_in(jax.random.fold_in(splits[5], part), 71), part),
        "grad_out": bell_draw(part_keys[3], (FRAMES, ROWS, COLS, D), 16.0, 96.0, ((0, 32), (1, 2))),
        "conv_taps": bell_draw(splits[4], (3, 3, D), 0.25, 4.0, (), jnp.float32),
    }


def mix_rows(padded, conv_taps, row_count, col_count, flipped):
    summed = jnp.zeros(padded.shape[:1] + (row_count, col_count, padded.shape[3]), jnp.float32)
    for row_off in range(3):
        for col_off in range(3):
            if flipped:
                window = padded[:, 2 - row_off:2 - row_off + row_count, 2 - col_off:2 - col_off + col_count]
            else:
                window = padded[:, row_off:row_off + row_count, col_off:col_off + col_count]
            summed = summed + conv_taps[row_off, col_off] * window
    return summed


def reference(query_pre, key_pre, value_pre, grad_out, conv_taps):
    frame_count, row_count, col_count, model_width = value_pre.shape
    head_count = HEADS
    head_size = HEAD_DIM
    split = (frame_count, row_count * col_count, head_count, head_size)
    highest = lax.Precision.HIGHEST
    value_pad = jnp.pad(value_pre.astype(jnp.float32), ((0, 0), (1, 1), (1, 1), (0, 0)))
    local = mix_rows(value_pad, conv_taps, row_count, col_count, False)
    queries = jnp.maximum(query_pre, 0).astype(jnp.float32).reshape(split)
    keys = jnp.maximum(key_pre, 0).astype(jnp.float32).reshape(split)
    values = value_pre.astype(jnp.float32).reshape(split)
    partial_value = jnp.einsum("fthe,fthd->fhed", keys, values, precision=highest)
    key_sum = jnp.sum(keys, axis=1)
    kv_state = jnp.cumsum(partial_value, axis=0)
    key_total = jnp.cumsum(key_sum, axis=0)
    numerator = jnp.einsum("fthe,fhed->fthd", queries, kv_state, precision=highest)
    denominator = jnp.einsum("fthe,fhe->fth", queries, key_total, precision=highest) + 1.0
    output_f32 = numerator / denominator[..., None]
    attended = (output_f32.reshape(value_pre.shape) + local).astype(jnp.bfloat16)
    cotangent = grad_out.astype(jnp.float32).reshape(split)
    grad_num = cotangent / denominator[..., None]
    grad_den = -jnp.sum(cotangent * output_f32, axis=-1) / denominator
    grad_query = jnp.einsum("fthd,fhed->fthe", grad_num, kv_state, precision=highest) + grad_den[..., None] * key_total[:, None]
    grad_partial = jnp.einsum("fthe,fthd->fhed", queries, grad_num, precision=highest)
    grad_keysum = jnp.einsum("fth,fthe->fhe", grad_den, queries, precision=highest)
    grad_state = jnp.flip(jnp.cumsum(jnp.flip(grad_partial, 0), axis=0), 0)
    grad_total = jnp.flip(jnp.cumsum(jnp.flip(grad_keysum, 0), axis=0), 0)
    grad_key = jnp.einsum("fthd,fhed->fthe", values, grad_state, precision=highest) + grad_total[:, None]
    grad_mixed = jnp.einsum("fthe,fhed->fthd", keys, grad_state, precision=highest).reshape(value_pre.shape)
    query_grad = jnp.where(query_pre > 0, grad_query.reshape(value_pre.shape), 0.0).astype(jnp.bfloat16)
    key_grad = jnp.where(key_pre > 0, grad_key.reshape(value_pre.shape), 0.0).astype(jnp.bfloat16)
    grad_pad = jnp.pad(grad_out.astype(jnp.float32), ((0, 0), (1, 1), (1, 1), (0, 0)))
    value_grad = (grad_mixed + mix_rows(grad_pad, conv_taps, row_count, col_count, True)).astype(jnp.bfloat16)
    cotangent_full = grad_out.astype(jnp.float32)
    tap_rows = []
    for row_off in range(3):
        tap_cols = []
        for col_off in range(3):
            window = value_pad[:, row_off:row_off + row_count, col_off:col_off + col_count]
            tap_cols.append(jnp.sum(cotangent_full * window, axis=(0, 1, 2)))
        tap_rows.append(jnp.stack(tap_cols))
    taps_grad = jnp.stack(tap_rows)
    return attended, query_grad, key_grad, value_grad, taps_grad
```

```python
import functools

import jax
import jax.numpy as jnp
from jax import lax
from jax.experimental import pallas as pl
from jax.experimental.pallas import tpu as pltpu
from jax.sharding import PartitionSpec as P

HEADS = 20
HD = 112
LN = 128
HC = 10
WC = HC * LN
NEAR = 4
ROWS = 1024
F32 = jnp.float32
BF = jnp.bfloat16
INTERPRET = False


def call(kernel, outs, *args):
    specs = [pl.BlockSpec(memory_space=pltpu.SMEM)]
    specs += [pl.BlockSpec(memory_space=pltpu.VMEM)] * (len(args) - 1)
    return pl.pallas_call(
        kernel,
        out_shape=[jax.ShapeDtypeStruct(s, d) for s, d in outs],
        in_specs=specs,
        out_specs=[pl.BlockSpec(memory_space=pltpu.VMEM)] * len(outs),
        interpret=INTERPRET,
    )(*args)


def lane(shape):
    return lax.broadcasted_iota(jnp.int32, shape, len(shape) - 1)


def halves(x):
    hi = x.astype(BF)
    return hi, (x - hi.astype(F32)).astype(BF)


def joined(hi, lo):
    return hi.astype(F32) + lo.astype(F32)


def mm(a, b, dims):
    return lax.dot_general(a, b, (dims, ((), ())), preferred_element_type=F32)


NN = ((1,), (0,))
NT = ((1,), (1,))
TN = ((0,), (0,))


def flag(cond):
    return jnp.where(cond, 1.0, 0.0).astype(F32)


def pack(ref, mats):
    last = mats[7]
    lanes = lane((HD, LN))
    for i in range(7):
        piece = pltpu.roll(last, HD - 16 * i, 1) if i < 7 else last
        ref[HD * i : HD * (i + 1), :] = jnp.where(lanes < HD, mats[i], piece)
    ref[HD * 7 : HD * 8, :] = mats[8]
    ref[HD * 8 : HD * 9, :] = mats[9]
    ref[HD * 9 : ROWS, :] = jnp.zeros((ROWS - HD * 9, LN), F32)


def unpack(ref):
    lanes = lane((HD, LN))
    mats, last = [], jnp.zeros((HD, LN), F32)
    for i in range(7):
        x = ref[HD * i : HD * (i + 1), :]
        mats.append(jnp.where(lanes < HD, x, 0.0))
        inside = (lanes >= 16 * i) & (lanes < 16 * i + 16)
        last = jnp.where(inside, pltpu.roll(x, 16 + 16 * i, 1), last)
    return mats + [last, ref[HD * 7 : HD * 8, :], ref[HD * 8 : HD * 9, :]]


def pad_rows(x):
    return jnp.concatenate([x, jnp.zeros((LN - HD, LN), x.dtype)], axis=0)


def heads_of(tile, width):
    out = []
    for h in range(HEADS):
        t, off = divmod(HD * h, LN)
        x = tile(t)
        if off:
            x = pltpu.roll(x, LN - off, 1)
        if off + HD > LN:
            y = pltpu.roll(tile(t + 1), LN - off, 1)
            x = jnp.where(lane(x.shape) < LN - off, x, y)
        out.append(jnp.where(lane(x.shape) < HD, x, 0.0))
    return out


def tiles_of(heads):
    out = []
    for t in range(-(-HEADS * HD // LN)):
        first, off = divmod(LN * t, HD)
        x = heads[first]
        if off:
            x = pltpu.roll(x, LN - off, 1)
        left = HD - off
        while left < LN and first + 1 < HEADS:
            first += 1
            y = pltpu.roll(heads[first], left, 1)
            x = jnp.where(lane(x.shape) < left, x, y)
            left += HD
        out.append(x)
    return out


def loader(ref, rows, width):
    cache = {}

    def tile(t):
        if t not in cache:
            n = min(LN, width - LN * t)
            x = ref[0:rows, LN * t : LN * t + n].astype(F32)
            if n < LN:
                x = jnp.concatenate([x, jnp.zeros((rows, LN - n), F32)], axis=1)
            cache[t] = x
        return cache[t]

    return tile


def spread_kernel(idx, q, k, v, g, taps, keep, send, taps_out):
    first = idx[0] == 0
    width = q.shape[1]
    rows = q.shape[0]
    for j, ref in enumerate((q, k, v, g)):
        heads = heads_of(loader(ref, rows, width), width)
        for i in range(HC):
            a, b = heads[i], heads[i + HC]
            if j < 2:
                a, b = jnp.maximum(a, 0.0), jnp.maximum(b, 0.0)
            keep[j, :, LN * i : LN * (i + 1)] = lax.select(first, a, b).astype(BF)
            send[j, :, LN * i : LN * (i + 1)] = lax.select(first, b, a).astype(BF)
    heads = heads_of(loader(taps, 9, width), width)
    for i in range(HC):
        taps_out[0:9, LN * i : LN * (i + 1)] = lax.select(first, heads[i], heads[i + HC])


def col(i):
    return slice(LN * i, LN * (i + 1))


def both(keep, recv, j, i):
    return jnp.concatenate([keep[j, :, col(i)], recv[j, :, col(i)]], axis=0)


def conv_kernel(idx, keep, recv, taps, local, gconv, taps_out):
    first = idx[0] == 0
    half = keep.shape[1]
    n = 2 * half
    cols = 32
    taps_out[...] = jnp.zeros_like(taps_out)
    pos = lax.broadcasted_iota(jnp.int32, (n, LN), 0) % cols
    zero_row = jnp.zeros((cols, LN), F32)

    def shifts(j, i):
        a, b = keep[j, :, col(i)].astype(F32), recv[j, :, col(i)].astype(F32)
        x = jnp.concatenate([lax.select(first, a, b), lax.select(first, b, a)], axis=0)
        before = jnp.where(pos == 0, 0.0, pltpu.roll(x, 1, 0))
        after = jnp.where(pos == cols - 1, 0.0, pltpu.roll(x, n - 1, 0))
        return before, x, after

    def up(u):
        return jnp.concatenate([zero_row, u[: n - cols]], axis=0)

    def down(u):
        return jnp.concatenate([u[cols:], zero_row], axis=0)

    def put(ref, x, i):
        ref[0:half, col(i)] = lax.select(first, x[:half], x[half:])
        ref[half:n, col(i)] = lax.select(first, x[half:], x[:half])

    for i in range(HC):
        w = taps[0:9, col(i)]
        vs, gs = shifts(2, i), shifts(3, i)
        u = [sum(w[3 * a + b : 3 * a + b + 1] * vs[b] for b in range(3)) for a in range(3)]
        put(local, up(u[0]) + u[1] + down(u[2]), i)
        u = [sum(w[3 * a + b : 3 * a + b + 1] * gs[2 - b] for b in range(3)) for a in range(3)]
        put(gconv, down(u[0]) + u[1] + up(u[2]), i)
        g = gs[1]
        for b in range(3):
            s = vs[b]
            for a, prod in enumerate((g[cols:] * s[: n - cols], g * s, g[: n - cols] * s[cols:])):
                r = 9 * i + 3 * a + b
                taps_out[r : r + 1, :] = jnp.sum(prod, axis=0, keepdims=True)


def rows_at(p, k, n):
    return pl.ds(pl.multiple_of((p ^ k) * n, n), n)


def partial_kernel(idx, keep, recv, own, ksum, a1, a2, a3, state):
    p = idx[1]
    ksum[...] = jnp.zeros_like(ksum)
    mats = []
    for i in range(HC):
        keys = both(keep, recv, 1, i)
        mats.append(mm(keys, both(keep, recv, 2, i), TN)[:HD])
        ksum[i : i + 1, :] = jnp.sum(keys.astype(F32), axis=0, keepdims=True)
    pack(state, mats)
    n = ROWS // NEAR
    own[...] = state[rows_at(p, 0, n), :]
    khi, klo = halves(ksum[...])
    for k, ref in enumerate((a1, a2, a3), 1):
        hi, lo = halves(state[rows_at(p, k, n), :])
        ref[0:n, :] = hi
        ref[n : 2 * n, :] = lo
        ref[2 * n : 2 * n + 16, :] = khi
        ref[2 * n + 16 : 2 * n + 32, :] = klo


def block_kernel(idx, own, ksum, a1, a2, a3, pay, kpre):
    p = idx[1]
    n = ROWS // NEAR
    total, ktot, kp = own[...], ksum[...], ksum[...]
    for k, ref in enumerate((a1, a2, a3), 1):
        total = total + joined(ref[0:n, :], ref[n : 2 * n, :])
        ks = joined(ref[2 * n : 2 * n + 16, :], ref[2 * n + 16 : 2 * n + 32, :])
        ktot = ktot + ks
        kp = kp + flag((p ^ k) <= p) * ks
    kpre[...] = kp
    khi, klo = halves(ktot)
    m = n // pay.shape[0]
    for b in range(pay.shape[0]):
        hi, lo = halves(total[m * b : m * (b + 1)])
        pay[b, 0:m, :] = hi
        pay[b, m : 2 * m, :] = lo
        pay[b, 2 * m : 2 * m + 16, :] = khi
        pay[b, 2 * m + 16 : 2 * m + 32, :] = klo


def reciprocal_of(q, kt, i):
    row = jnp.broadcast_to(kt[i : i + 1, :], (LN, LN))
    hi, lo = halves(row)
    den = mm(jnp.concatenate([q, q], axis=1), jnp.concatenate([hi, lo], axis=1), NT)
    return 1.0 / (den + 1.0)


def turn_kernel(idx, got, kpre, keep, recv, down, kt, own, c1, c2, c3, state):
    p, mine = idx[1], idx[2]
    nb = got.shape[0]
    n = ROWS // NEAR
    m = n // nb
    run, key_total = jnp.zeros((m, LN), F32), kpre[...]
    for b in range(nb):
        hi, lo = halves(run)
        down[b, 0:m, :] = hi
        down[b, m : 2 * m, :] = lo
        run = run + joined(got[b, 0:m, :], got[b, m : 2 * m, :])
        ks = joined(got[b, 2 * m : 2 * m + 16, :], got[b, 2 * m + 16 : 2 * m + 32, :])
        key_total = key_total + flag(b < mine) * ks
    kt[...] = key_total
    mats = []
    for i in range(HC):
        q = both(keep, recv, 0, i)
        scaled = both(keep, recv, 3, i).astype(F32) * reciprocal_of(q, key_total, i)
        hi, lo = halves(scaled)
        x = mm(q, jnp.concatenate([hi, lo], axis=1), TN)[:HD]
        mats.append(x[:, :LN] + x[:, LN:])
    pack(state, mats)
    own[...] = state[rows_at(p, 0, n), :]
    for k, ref in enumerate((c1, c2, c3), 1):
        ref[...] = state[rows_at(p, k, n), :].astype(BF)


def back_block_kernel(idx, own, c1, c2, c3, down, taps, pay):
    nb = pay.shape[0]
    m = ROWS // NEAR // nb
    total = own[...]
    for ref in (c1, c2, c3):
        total = total + ref[...].astype(F32)
    for b in range(nb):
        pay[b, 0 : 2 * m, :] = down[b]
        pay[b, 2 * m : 3 * m, :] = total[m * b : m * (b + 1)].astype(BF)
        hi, lo = halves(taps[16 * b : 16 * (b + 1), :])
        pay[b, 3 * m : 3 * m + 16, :] = hi
        pay[b, 3 * m + 16 : 3 * m + 32, :] = lo


def four_rows(x):
    hi = x.astype(BF).astype(F32)
    return jnp.concatenate([hi, x - hi, jnp.zeros((8, LN), F32)], axis=0).astype(BF)


def of_four(x):
    x = x.astype(F32)
    return x[0:4] + x[4:8]


def prefix_kernel(idx, got, own, a1, a2, a3, s_own, e1, e2, e3, taps_own, back, taps):
    p = idx[1]
    nb = got.shape[0]
    n = ROWS // NEAR
    m = n // nb
    base = jnp.concatenate([joined(got[b, 0:m, :], got[b, m : 2 * m, :]) for b in range(nb)], axis=0)
    run = jnp.zeros((m, LN), F32)
    t = jnp.zeros((16, LN), F32)
    for b in reversed(range(nb)):
        back[b] = run.astype(BF)
        run = run + got[b, 2 * m : 3 * m, :].astype(F32)
        t = t + joined(got[b, 3 * m : 3 * m + 16, :], got[b, 3 * m + 16 : 3 * m + 32, :])
    for j in range(NEAR):
        taps[j] = t[4 * j : 4 * (j + 1)]
    parts = [own[...]] + [joined(r[0:n, :], r[n : 2 * n, :]) for r in (a1, a2, a3)]
    for k, ref in enumerate((s_own, e1, e2, e3)):
        x = base
        for j in range(NEAR):
            x = x + flag((p ^ j) <= (p ^ k)) * parts[j]
        if k == 0:
            ref[...] = x
        else:
            hi, lo = halves(x)
            ref[0:n, :] = hi
            ref[n : 2 * n, :] = lo
            ref[2 * n : 2 * n + 16, :] = four_rows(taps[p ^ k])
    taps_own[...] = taps[p]


def attend_kernel(
    idx, e1, e2, e3, s_own, kt, keep, recv, local, taps_own, back, att, query, pay, gks_out, state, gks
):
    p = idx[1]
    nb = pay.shape[0]
    n = ROWS // NEAR
    m = n // nb
    half = keep.shape[1]
    state[rows_at(p, 0, n), :] = s_own[...]
    taps = taps_own[...]
    for k, ref in enumerate((e1, e2, e3), 1):
        state[rows_at(p, k, n), :] = joined(ref[0:n, :], ref[n : 2 * n, :])
        taps = taps + of_four(ref[2 * n : 2 * n + 16, :])
    mats = unpack(state)
    key_total = kt[...]
    gks[...] = jnp.zeros_like(gks)
    ones = jnp.ones((2 * LN, LN), BF)
    for i in range(HC):
        q, g = both(keep, recv, 0, i), both(keep, recv, 3, i)
        hi, lo = halves(pad_rows(mats[i]))
        recip = reciprocal_of(q, key_total, i)
        out = mm(jnp.concatenate([q, q], axis=1), jnp.concatenate([hi, lo], axis=0), NN) * recip
        x = (out + local[:, col(i)]).astype(BF)
        att[0, :, col(i)] = x[:half]
        att[1, :, col(i)] = x[half:]
        ghi, glo = halves(g.astype(F32) * out)
        gden = -mm(jnp.concatenate([ghi, glo], axis=1), ones, NN) * recip
        gs = mm(jnp.concatenate([g, g], axis=1), jnp.concatenate([hi, lo], axis=1), NT)
        qf = q.astype(F32)
        x = jnp.where(qf > 0.0, gs * recip + gden * key_total[i : i + 1, :], 0.0).astype(BF)
        query[0, :, col(i)] = x[:half]
        query[1, :, col(i)] = x[half:]
        gks[i : i + 1, :] = jnp.sum(gden * qf, axis=0, keepdims=True)
    gks_out[...] = gks[...]
    khi, klo = halves(gks[...])
    four = four_rows(taps)
    for b in range(nb):
        pay[b, 0:m, :] = back[b]
        pay[b, m : m + 16, :] = khi
        pay[b, m + 16 : m + 32, :] = klo
        pay[b, m + 32 : m + 48, :] = four


def suffix_kernel(idx, got, own, c1, c2, c3, gks, g_own, gt_own, taps_own, g1, g2, g3):
    p, mine = idx[1], idx[2]
    nb = got.shape[0]
    n = ROWS // NEAR
    m = n // nb
    base = jnp.concatenate([got[b, 0:m, :].astype(F32) for b in range(nb)], axis=0)
    later = jnp.zeros((16, LN), F32)
    for b in range(nb):
        ks = joined(got[b, m : m + 16, :], got[b, m + 16 : m + 32, :])
        later = later + flag(b > mine) * ks
    taps = jnp.concatenate([of_four(got[b, m + 32 : m + 48, :]) for b in range(nb)], axis=0)
    taps_own[...] = taps
    thi, tlo = halves(taps)
    parts = [own[...]] + [r[...].astype(F32) for r in (c1, c2, c3)]
    nt = taps.shape[0]
    for k, ref in enumerate((g_own, g1, g2, g3)):
        x = base
        for j in range(NEAR):
            x = x + flag((p ^ j) >= (p ^ k)) * parts[j]
        if k == 0:
            ref[...] = x
            gt_own[...] = later + gks[...]
        else:
            ref[0:n, :] = x.astype(BF)
            hi, lo = halves(later + flag(p >= (p ^ k)) * gks[...])
            ref[n : n + 16, :] = hi
            ref[n + 16 : n + 32, :] = lo
            ref[n + 32 : n + 32 + nt, :] = thi
            ref[n + 32 + nt : n + 32 + 2 * nt, :] = tlo


def finish_kernel(
    idx, g1, g2, g3, g_own, gt_own, taps_own, keep, recv, gconv, key, value, taps, state
):
    p = idx[1]
    n = ROWS // NEAR
    half = keep.shape[1]
    nt = taps_own.shape[0]
    state[rows_at(p, 0, n), :] = g_own[...]
    taps[p] = joined(*halves(taps_own[...]))
    total = gt_own[...]
    for k, ref in enumerate((g1, g2, g3), 1):
        state[rows_at(p, k, n), :] = ref[0:n, :].astype(F32)
        total = total + joined(ref[n : n + 16, :], ref[n + 16 : n + 32, :])
        taps[p ^ k] = joined(ref[n + 32 : n + 32 + nt, :], ref[n + 32 + nt : n + 32 + 2 * nt, :])
    mats = unpack(state)
    for i in range(HC):
        keys, v = both(keep, recv, 1, i), both(keep, recv, 2, i)
        hi, lo = halves(pad_rows(mats[i]))
        gk = mm(jnp.concatenate([v, v], axis=1), jnp.concatenate([hi, lo], axis=1), NT)
        x = jnp.where(keys.astype(F32) > 0.0, gk + total[i : i + 1, :], 0.0).astype(BF)
        key[0, :, col(i)] = x[:half]
        key[1, :, col(i)] = x[half:]
        gm = mm(jnp.concatenate([keys, keys], axis=1), jnp.concatenate([hi, lo], axis=0), NN)
        x = (gm + gconv[:, col(i)]).astype(BF)
        value[0, :, col(i)] = x[:half]
        value[1, :, col(i)] = x[half:]


def gather_heads(first, mine, other, ref):
    heads = [lax.select(first, mine(i), other(i)) for i in range(HC)]
    heads += [lax.select(first, other(i), mine(i)) for i in range(HC)]
    width = ref.shape[1]
    rows = ref.shape[0]
    for t, x in enumerate(tiles_of(heads)):
        n = min(LN, width - LN * t)
        ref[:, LN * t : LN * t + n] = x[:rows, :n].astype(ref.dtype)


def merge_kernel(idx, mine_a, mine_b, other_a, other_b, out_a, out_b):
    first = idx[0] == 0
    for mine, other, ref in ((mine_a, other_a, out_a), (mine_b, other_b, out_b)):
        gather_heads(
            first,
            lambda i: mine[0, :, col(i)].astype(F32),
            lambda i: other[:, col(i)].astype(F32),
            ref,
        )


def merge_taps_kernel(
    idx, mine_a, mine_b, other_a, other_b, mine_t, other_t, out_a, out_b, out_t, mine_s, other_s
):
    merge_kernel(idx, mine_a, mine_b, other_a, other_b, out_a, out_b)
    for src, dst in ((mine_t, mine_s), (other_t, other_s)):
        for u in range(-(-9 * HC // 4)):
            j, b = u % NEAR, u // NEAR
            dst[4 * u : 4 * (u + 1), :] = src[j, 4 * b : 4 * (b + 1), :]
    gather_heads(
        idx[0] == 0, lambda i: mine_s[9 * i : 9 * (i + 1), :], lambda i: other_s[9 * i : 9 * (i + 1), :], out_t
    )


def with_scratch(kernel, outs, scratch, *args):
    specs = [pl.BlockSpec(memory_space=pltpu.SMEM)]
    specs += [pl.BlockSpec(memory_space=pltpu.VMEM)] * (len(args) - 1)
    return pl.pallas_call(
        kernel,
        out_shape=[jax.ShapeDtypeStruct(s, d) for s, d in outs],
        in_specs=specs,
        out_specs=[pl.BlockSpec(memory_space=pltpu.VMEM)] * len(outs),
        scratch_shapes=[pltpu.VMEM(s, d) for s, d in scratch],
        interpret=INTERPRET,
    )(*args)


def shards(query_pre, key_pre, value_pre, grad_out, conv_taps):
    shape = value_pre.shape
    width = shape[-1]
    t = shape[0] * shape[1] * shape[2]
    frames = lax.axis_size("tm")
    nb = frames // NEAR
    place = lax.axis_index("tm")
    core = lax.axis_index("space")
    idx = jnp.stack([core, place % NEAR, place // NEAR]).astype(jnp.int32)
    swap = [(0, 1), (1, 0)]
    across = [[j + NEAR * b for b in range(nb)] for j in range(NEAR)]

    def over(x):
        return lax.ppermute(x, "space", swap)

    def near(arrays):
        return [
            lax.ppermute(a, "tm", [(i, i ^ k) for i in range(frames)])
            for k, a in enumerate(arrays, 1)
        ]

    def far(x):
        return lax.all_to_all(x, "tm", 0, 0, axis_index_groups=across, tiled=True)

    n = ROWS // NEAR
    m = n // nb
    flat = [x.reshape(t, width) for x in (query_pre, key_pre, value_pre, grad_out)]
    half = ((4, t, WC), BF)
    keep, send, taps = call(
        spread_kernel, [half, half, ((16, WC), F32)], idx, *flat, conv_taps.reshape(9, width)
    )
    recv = over(send)

    share = ((n, LN), F32)
    small = ((16, LN), F32)
    state = ((ROWS, LN), F32)
    own_b, ksum, *out = with_scratch(
        partial_kernel, [share, small] + [((2 * n + 32, LN), BF)] * 3, [state], idx, keep, recv
    )
    got_a = near(out)
    local, gconv, taps_part = call(
        conv_kernel, [((2 * t, WC), F32)] * 2 + [((LN, LN), F32)], idx, keep, recv, taps
    )
    pay, kpre = call(
        block_kernel, [((nb, 2 * m + 32, LN), BF), small], idx, own_b, ksum, *got_a
    )
    got = far(pay)
    down, kt, own_d, *out = with_scratch(
        turn_kernel,
        [((nb, 2 * m, LN), BF), small, share] + [((n, LN), BF)] * 3,
        [state],
        idx, got, kpre, keep, recv,
    )
    got_c = near(out)
    (pay,) = call(
        back_block_kernel, [((nb, 3 * m + 32, LN), BF)], idx, own_d, *got_c, down, taps_part
    )
    got = far(pay)
    s_own, e1, e2, e3, taps_own, back = with_scratch(
        prefix_kernel,
        [share] + [((2 * n + 16, LN), BF)] * 3 + [((4, LN), F32), ((nb, m, LN), BF)],
        [((NEAR, 4, LN), F32)],
        idx, got, own_b, *got_a,
    )
    got_e = near((e1, e2, e3))
    pair = ((2, t, WC), BF)
    att, query, pay, gks = with_scratch(
        attend_kernel,
        [pair, pair, ((nb, m + 48, LN), BF), small],
        [state, small],
        idx, *got_e, s_own, kt, keep, recv, local, taps_own, back,
    )
    got = far(pay)
    g_own, gt_own, taps_own, *out = call(
        suffix_kernel,
        [share, small, ((4 * nb, LN), F32)] + [((n + 32 + 8 * nb, LN), BF)] * 3,
        idx, got, own_d, *got_c, gks,
    )
    got_g = near(out)
    whole = ((t, width), BF)
    attended, query_grad = call(
        merge_kernel, [whole, whole], idx, att, query, over(att[1]), over(query[1])
    )
    key, value, taps_all = with_scratch(
        finish_kernel,
        [pair, pair, ((NEAR, 4 * nb, LN), F32)],
        [state],
        idx, *got_g, g_own, gt_own, taps_own, keep, recv, gconv,
    )
    key_grad, value_grad, taps_grad = with_scratch(
        merge_taps_kernel,
        [whole, whole, ((9, width), F32)],
        [((LN, LN), F32)] * 2,
        idx, key, value, over(key[1]), over(value[1]), taps_all, over(taps_all),
    )
    return (
        attended.reshape(shape),
        query_grad.reshape(shape),
        key_grad.reshape(shape),
        value_grad.reshape(shape),
        taps_grad.reshape(conv_taps.shape),
    )


def solution(mesh):
    frame = P(("groups", "tm"), "space", None, None)
    return jax.shard_map(
        shards,
        mesh=mesh,
        in_specs=(frame, frame, frame, frame, P()),
        out_specs=(frame, frame, frame, frame, P("groups", None, None)),
        check_vma=False,
    )
```

```python
import functools

import jax
import jax.numpy as jnp
from jax import lax
from jax.experimental import pallas as pl
from jax.experimental.pallas import tpu as pltpu
from jax.sharding import PartitionSpec as P

HEADS = 20
HD = 112
LN = 128
HC = 10
WC = HC * LN
NEAR = 4
ROWS = 1024
F32 = jnp.float32
BF = jnp.bfloat16
INTERPRET = False
VMEM_LIMIT = 16 << 20


def call(kernel, outs, *args, scratch=(), us=1):
    return pl.pallas_call(
        kernel,
        out_shape=[jax.ShapeDtypeStruct(s, d) for s, d in outs],
        in_specs=[pl.BlockSpec(memory_space=pltpu.VMEM)] * len(args),
        out_specs=[pl.BlockSpec(memory_space=pltpu.VMEM)] * len(outs),
        scratch_shapes=[pltpu.VMEM(s, d) for s, d in scratch],
        interpret=INTERPRET,
        cost_estimate=pl.CostEstimate(flops=us * 10**9, bytes_accessed=10**6, transcendentals=0),
        compiler_params=pltpu.CompilerParams(vmem_limit_bytes=VMEM_LIMIT),
    )(*args)


def place():
    frame = lax.axis_index("tm")
    return lax.axis_index("space"), lax.rem(frame, NEAR), lax.div(frame, NEAR)


def lane(shape):
    return lax.broadcasted_iota(jnp.int32, shape, len(shape) - 1)


def halves(x):
    hi = x.astype(BF)
    return hi, (x - hi.astype(F32)).astype(BF)


def joined(hi, lo):
    return hi.astype(F32) + lo.astype(F32)


def mm(a, b, dims):
    return lax.dot_general(a, b, (dims, ((), ())), preferred_element_type=F32)


NN = ((1,), (0,))
NT = ((1,), (1,))
TN = ((0,), (0,))


def flag(cond):
    return jnp.where(cond, 1.0, 0.0).astype(F32)


def pack(ref, mats):
    last = mats[7]
    lanes = lane((HD, LN))
    for i in range(7):
        piece = pltpu.roll(last, HD - 16 * i, 1) if i < 7 else last
        ref[HD * i : HD * (i + 1), :] = jnp.where(lanes < HD, mats[i], piece)
    ref[HD * 7 : HD * 8, :] = mats[8]
    ref[HD * 8 : HD * 9, :] = mats[9]
    ref[HD * 9 : ROWS, :] = jnp.zeros((ROWS - HD * 9, LN), F32)


def unpack(ref):
    lanes = lane((HD, LN))
    mats, last = [], jnp.zeros((HD, LN), F32)
    for i in range(7):
        x = ref[HD * i : HD * (i + 1), :]
        mats.append(jnp.where(lanes < HD, x, 0.0))
        inside = (lanes >= 16 * i) & (lanes < 16 * i + 16)
        last = jnp.where(inside, pltpu.roll(x, 16 + 16 * i, 1), last)
    return mats + [last, ref[HD * 7 : HD * 8, :], ref[HD * 8 : HD * 9, :]]


def pad_rows(x):
    return jnp.concatenate([x, jnp.zeros((LN - HD, LN), x.dtype)], axis=0)


def heads_of(tile):
    out = []
    for h in range(HEADS):
        t, off = divmod(HD * h, LN)
        x = tile(t)
        if off:
            x = pltpu.roll(x, LN - off, 1)
        if off + HD > LN:
            y = pltpu.roll(tile(t + 1), LN - off, 1)
            x = jnp.where(lane(x.shape) < LN - off, x, y)
        out.append(jnp.where(lane(x.shape) < HD, x, 0.0))
    return out


def tiles_of(heads):
    out = []
    for t in range(-(-HEADS * HD // LN)):
        first, off = divmod(LN * t, HD)
        x = heads[first]
        if off:
            x = pltpu.roll(x, LN - off, 1)
        left = HD - off
        while left < LN and first + 1 < HEADS:
            first += 1
            y = pltpu.roll(heads[first], left, 1)
            x = jnp.where(lane(x.shape) < left, x, y)
            left += HD
        out.append(x)
    return out


def loader(ref, rows, width):
    cache = {}

    def tile(t):
        if t not in cache:
            n = min(LN, width - LN * t)
            x = ref[0:rows, LN * t : LN * t + n].astype(F32)
            if n < LN:
                x = jnp.concatenate([x, jnp.zeros((rows, LN - n), F32)], axis=1)
            cache[t] = x
        return cache[t]

    return tile


def spread(refs, relu, keep, send):
    first = place()[0] == 0
    for j, ref in enumerate(refs):
        rows, width = ref.shape
        heads = heads_of(loader(ref, rows, width))
        for i in range(HC):
            a, b = heads[i], heads[i + HC]
            if relu[j]:
                a, b = jnp.maximum(a, 0.0), jnp.maximum(b, 0.0)
            keep[j, :, col(i)] = lax.select(first, a, b).astype(BF)
            send[j, :, col(i)] = lax.select(first, b, a).astype(BF)


def spread_kv_kernel(k, v, keep, send):
    spread((k, v), (True, False), keep, send)


def spread_qg_kernel(q, g, taps, after, keep, send, taps_out):
    first = place()[0] == 0
    spread((q, g), (True, False), keep, send)
    for a in range(3):
        heads = heads_of(loader(taps.at[a], 3, taps.shape[2]))
        for i in range(HC):
            taps_out[a, :, col(i)] = lax.select(first, heads[i], heads[i + HC])


def col(i):
    return slice(LN * i, LN * (i + 1))


def both(keep, recv, j, i):
    return jnp.concatenate([keep[j, :, col(i)], recv[j, :, col(i)]], axis=0)


def conv_kernel(keep_v, recv_v, keep_g, recv_g, taps, local, gc_mine, gc_other, taps_out):
    first = place()[0] == 0
    half = keep_v.shape[1]
    n = 2 * half
    cols = 32
    taps_out[...] = jnp.zeros_like(taps_out)
    pos = lax.broadcasted_iota(jnp.int32, (n, LN), 0) % cols
    zero_row = jnp.zeros((cols, LN), F32)

    def shifts(keep, recv, i):
        a, b = keep[1, :, col(i)].astype(F32), recv[1, :, col(i)].astype(F32)
        x = jnp.concatenate([lax.select(first, a, b), lax.select(first, b, a)], axis=0)
        before = jnp.where(pos == 0, 0.0, pltpu.roll(x, 1, 0))
        after = jnp.where(pos == cols - 1, 0.0, pltpu.roll(x, n - 1, 0))
        return before, x, after

    def up(u):
        return jnp.concatenate([zero_row, u[: n - cols]], axis=0)

    def down(u):
        return jnp.concatenate([u[cols:], zero_row], axis=0)

    def put(mine, other, x, i):
        mine[:, col(i)] = lax.select(first, x[:half], x[half:])
        other[:, col(i)] = lax.select(first, x[half:], x[:half])

    for i in range(HC):
        w = [taps[a, :, col(i)] for a in range(3)]
        vs, gs = shifts(keep_v, recv_v, i), shifts(keep_g, recv_g, i)
        u = [sum(w[a][b : b + 1] * vs[b] for b in range(3)) for a in range(3)]
        put(local.at[0:half], local.at[half:n], up(u[0]) + u[1] + down(u[2]), i)
        u = [sum(w[a][b : b + 1] * gs[2 - b] for b in range(3)) for a in range(3)]
        put(gc_mine, gc_other, down(u[0]) + u[1] + up(u[2]), i)
        g = gs[1]
        for b in range(3):
            s = vs[b]
            for a, prod in enumerate((g[cols:] * s[: n - cols], g * s, g[: n - cols] * s[cols:])):
                r = 9 * i + 3 * a + b
                taps_out[r : r + 1, :] = jnp.sum(prod, axis=0, keepdims=True)


def rows_at(p, k, n):
    return pl.ds(pl.multiple_of((p ^ k) * n, n), n)


def partial_kernel(keep, recv, own, ksum, a1, a2, a3, state):
    p = place()[1]
    ksum[...] = jnp.zeros_like(ksum)
    mats = []
    for i in range(HC):
        keys = both(keep, recv, 0, i)
        mats.append(mm(keys, both(keep, recv, 1, i), TN)[:HD])
        ksum[i : i + 1, :] = jnp.sum(keys.astype(F32), axis=0, keepdims=True)
    pack(state, mats)
    n = ROWS // NEAR
    own[...] = state[rows_at(p, 0, n), :]
    khi, klo = halves(ksum[...])
    for k, ref in enumerate((a1, a2, a3), 1):
        hi, lo = halves(state[rows_at(p, k, n), :])
        ref[0:n, :] = hi
        ref[n : 2 * n, :] = lo
        ref[2 * n : 2 * n + 16, :] = khi
        ref[2 * n + 16 : 2 * n + 32, :] = klo


def block_kernel(own, ksum, a1, a2, a3, pay, kpre):
    p = place()[1]
    n = ROWS // NEAR
    total, ktot, kp = own[...], ksum[...], ksum[...]
    for k, ref in enumerate((a1, a2, a3), 1):
        total = total + joined(ref[0:n, :], ref[n : 2 * n, :])
        ks = joined(ref[2 * n : 2 * n + 16, :], ref[2 * n + 16 : 2 * n + 32, :])
        ktot = ktot + ks
        kp = kp + flag((p ^ k) <= p) * ks
    kpre[...] = kp
    khi, klo = halves(ktot)
    m = n // pay.shape[0]
    for b in range(pay.shape[0]):
        hi, lo = halves(total[m * b : m * (b + 1)])
        pay[b, 0:m, :] = hi
        pay[b, m : 2 * m, :] = lo
        pay[b, 2 * m : 2 * m + 16, :] = khi
        pay[b, 2 * m + 16 : 2 * m + 32, :] = klo


def reciprocal_of(q, kt, i):
    row = jnp.broadcast_to(kt[i : i + 1, :], (LN, LN))
    hi, lo = halves(row)
    den = mm(jnp.concatenate([q, q], axis=1), jnp.concatenate([hi, lo], axis=1), NT)
    return 1.0 / (den + 1.0)


def turn_kernel(got, kpre, keep, recv, down, kt, own, c1, c2, c3, state):
    _, p, mine = place()
    nb = got.shape[0]
    n = ROWS // NEAR
    m = n // nb
    run, key_total = jnp.zeros((m, LN), F32), kpre[...]
    for b in range(nb):
        hi, lo = halves(run)
        down[b, 0:m, :] = hi
        down[b, m : 2 * m, :] = lo
        run = run + joined(got[b, 0:m, :], got[b, m : 2 * m, :])
        ks = joined(got[b, 2 * m : 2 * m + 16, :], got[b, 2 * m + 16 : 2 * m + 32, :])
        key_total = key_total + flag(b < mine) * ks
    kt[...] = key_total
    mats = []
    for i in range(HC):
        q = both(keep, recv, 0, i)
        scaled = both(keep, recv, 1, i).astype(F32) * reciprocal_of(q, key_total, i)
        hi, lo = halves(scaled)
        x = mm(q, jnp.concatenate([hi, lo], axis=1), TN)[:HD]
        mats.append(x[:, :LN] + x[:, LN:])
    pack(state, mats)
    own[...] = state[rows_at(p, 0, n), :]
    for k, ref in enumerate((c1, c2, c3), 1):
        ref[...] = state[rows_at(p, k, n), :].astype(BF)


def back_block_kernel(own, c1, c2, c3, down, taps, pay):
    nb = pay.shape[0]
    m = ROWS // NEAR // nb
    total = own[...]
    for ref in (c1, c2, c3):
        total = total + ref[...].astype(F32)
    for b in range(nb):
        pay[b, 0 : 2 * m, :] = down[b]
        pay[b, 2 * m : 3 * m, :] = total[m * b : m * (b + 1)].astype(BF)
        hi, lo = halves(taps[16 * b : 16 * (b + 1), :])
        pay[b, 3 * m : 3 * m + 16, :] = hi
        pay[b, 3 * m + 16 : 3 * m + 32, :] = lo


def four_rows(x):
    hi = x.astype(BF).astype(F32)
    return jnp.concatenate([hi, x - hi, jnp.zeros((8, LN), F32)], axis=0).astype(BF)


def of_four(x):
    x = x.astype(F32)
    return x[0:4] + x[4:8]


def prefix_kernel(got, own, a1, a2, a3, s_own, e1, e2, e3, taps_own, back, taps):
    p = place()[1]
    nb = got.shape[0]
    n = ROWS // NEAR
    m = n // nb
    base = jnp.concatenate([joined(got[b, 0:m, :], got[b, m : 2 * m, :]) for b in range(nb)], axis=0)
    run = jnp.zeros((m, LN), F32)
    t = jnp.zeros((16, LN), F32)
    for b in reversed(range(nb)):
        back[b] = run.astype(BF)
        run = run + got[b, 2 * m : 3 * m, :].astype(F32)
        t = t + joined(got[b, 3 * m : 3 * m + 16, :], got[b, 3 * m + 16 : 3 * m + 32, :])
    for j in range(NEAR):
        taps[j] = t[4 * j : 4 * (j + 1)]
    parts = [own[...]] + [joined(r[0:n, :], r[n : 2 * n, :]) for r in (a1, a2, a3)]
    for k, ref in enumerate((s_own, e1, e2, e3)):
        x = base
        for j in range(NEAR):
            x = x + flag((p ^ j) <= (p ^ k)) * parts[j]
        if k == 0:
            ref[...] = x
        else:
            hi, lo = halves(x)
            ref[0:n, :] = hi
            ref[n : 2 * n, :] = lo
            ref[2 * n : 2 * n + 16, :] = four_rows(taps[p ^ k])
    taps_own[...] = taps[p]


def attend_kernel(
    e1, e2, e3, s_own, kt, keep, recv, local, taps_own, back, mine, other, pay, gks_out, state, gks
):
    p = place()[1]
    nb = pay.shape[0]
    n = ROWS // NEAR
    m = n // nb
    half = keep.shape[1]
    state[rows_at(p, 0, n), :] = s_own[...]
    taps = taps_own[...]
    for k, ref in enumerate((e1, e2, e3), 1):
        state[rows_at(p, k, n), :] = joined(ref[0:n, :], ref[n : 2 * n, :])
        taps = taps + of_four(ref[2 * n : 2 * n + 16, :])
    mats = unpack(state)
    key_total = kt[...]
    gks[...] = jnp.zeros_like(gks)
    ones = jnp.ones((2 * LN, LN), BF)
    for i in range(HC):
        q, g = both(keep, recv, 0, i), both(keep, recv, 1, i)
        hi, lo = halves(pad_rows(mats[i]))
        recip = reciprocal_of(q, key_total, i)
        out = mm(jnp.concatenate([q, q], axis=1), jnp.concatenate([hi, lo], axis=0), NN) * recip
        x = (out + local[:, col(i)]).astype(BF)
        mine[0, :, col(i)] = x[:half]
        other[0, :, col(i)] = x[half:]
        ghi, glo = halves(g.astype(F32) * out)
        gden = -mm(jnp.concatenate([ghi, glo], axis=1), ones, NN) * recip
        gs = mm(jnp.concatenate([g, g], axis=1), jnp.concatenate([hi, lo], axis=1), NT)
        qf = q.astype(F32)
        x = jnp.where(qf > 0.0, gs * recip + gden * key_total[i : i + 1, :], 0.0).astype(BF)
        mine[1, :, col(i)] = x[:half]
        other[1, :, col(i)] = x[half:]
        gks[i : i + 1, :] = jnp.sum(gden * qf, axis=0, keepdims=True)
    gks_out[...] = gks[...]
    khi, klo = halves(gks[...])
    four = four_rows(taps)
    for b in range(nb):
        pay[b, 0:m, :] = back[b]
        pay[b, m : m + 16, :] = khi
        pay[b, m + 16 : m + 32, :] = klo
        pay[b, m + 32 : m + 48, :] = four


def suffix_kernel(got, own, c1, c2, c3, gks, g0, g1, g2, g3):
    _, p, mine = place()
    nb = got.shape[0]
    n = ROWS // NEAR
    m = n // nb
    base = jnp.concatenate([got[b, 0:m, :].astype(F32) for b in range(nb)], axis=0)
    later = jnp.zeros((16, LN), F32)
    for b in range(nb):
        ks = joined(got[b, m : m + 16, :], got[b, m + 16 : m + 32, :])
        later = later + flag(b > mine) * ks
    taps = jnp.concatenate([of_four(got[b, m + 32 : m + 48, :]) for b in range(nb)], axis=0)
    thi, tlo = halves(taps)
    parts = [own[...]] + [r[...].astype(F32) for r in (c1, c2, c3)]
    nt = taps.shape[0]
    for k, ref in enumerate((g0, g1, g2, g3)):
        x = base
        for j in range(NEAR):
            x = x + flag((p ^ j) >= (p ^ k)) * parts[j]
        ref[0:n, :] = x.astype(BF)
        hi, lo = halves(later + flag(p >= (p ^ k)) * gks[...])
        ref[n : n + 16, :] = hi
        ref[n + 16 : n + 32, :] = lo
        ref[n + 32 : n + 32 + nt, :] = thi
        ref[n + 32 + nt : n + 32 + 2 * nt, :] = tlo


def assembled(refs, state, taps):
    p = place()[1]
    n = ROWS // NEAR
    nt = (refs[0].shape[0] - n - 32) // 2
    total = jnp.zeros((16, LN), F32)
    for k, ref in enumerate(refs):
        state[rows_at(p, k, n), :] = ref[0:n, :].astype(F32)
        total = total + joined(ref[n : n + 16, :], ref[n + 16 : n + 32, :])
        part = joined(ref[n + 32 : n + 32 + nt, :], ref[n + 32 + nt : n + 32 + 2 * nt, :])
        for b in range(nt // 4):
            taps[b, p ^ k] = part[4 * b : 4 * (b + 1)]
    return unpack(state), total


def finish_kernel(
    g0, g1, g2, g3, o0, o1, o2, o3, keep, send, gc_mine, gc_other, key, value, taps, state, taps_a, taps_b
):
    first = place()[0] == 0
    sides = []
    for refs, tokens, conv, scratch in (
        ((g0, g1, g2, g3), keep, gc_mine, taps_a),
        ((o0, o1, o2, o3), send, gc_other, taps_b),
    ):
        mats, total = assembled(refs, state, scratch)
        keys_out, values_out, taps_out = [], [], []
        for i in range(HC):
            keys, v = tokens[0, :, col(i)], tokens[1, :, col(i)]
            hi, lo = halves(pad_rows(mats[i]))
            gk = mm(jnp.concatenate([v, v], axis=1), jnp.concatenate([hi, lo], axis=1), NT)
            keys_out.append(jnp.where(keys.astype(F32) > 0.0, gk + total[i : i + 1, :], 0.0))
            gm = mm(jnp.concatenate([keys, keys], axis=1), jnp.concatenate([hi, lo], axis=0), NN)
            values_out.append(gm + conv[:, col(i)])
        sides.append((keys_out, values_out))
    for j, ref in enumerate((key, value)):
        gather_heads(first, sides[0][j], sides[1][j], ref)
    for a in range(3):
        rows = []
        for scratch in (taps_a, taps_b):
            heads = []
            for i in range(HC):
                lines = []
                for b in range(3):
                    r = 9 * i + 3 * a + b
                    lines.append(scratch[r // 16, (r % 16) // 4, r % 4 : r % 4 + 1, :])
                heads.append(jnp.concatenate(lines, axis=0))
            rows.append(heads)
        gather_heads(first, rows[0], rows[1], taps.at[a])


def gather_heads(first, mine, other, ref):
    heads = [lax.select(first, mine[i], other[i]) for i in range(HC)]
    heads += [lax.select(first, other[i], mine[i]) for i in range(HC)]
    width = ref.shape[1]
    for t, x in enumerate(tiles_of(heads)):
        n = min(LN, width - LN * t)
        ref[:, LN * t : LN * t + n] = x[:, :n].astype(ref.dtype)


def merge_kernel(mine, other, out_a, out_b):
    first = place()[0] == 0
    for j, ref in enumerate((out_a, out_b)):
        heads = [[x[j, :, col(i)].astype(F32) for i in range(HC)] for x in (mine, other)]
        gather_heads(first, heads[0], heads[1], ref)


def shards(query_pre, key_pre, value_pre, grad_out, conv_taps):
    shape = value_pre.shape
    width = shape[-1]
    t = shape[0] * shape[1] * shape[2]
    frames = lax.axis_size("tm")
    nb = frames // NEAR
    across = [[j + NEAR * b for b in range(nb)] for j in range(NEAR)]

    def over(x):
        return lax.ppermute(x, "space", [(0, 1), (1, 0)])

    def near(arrays):
        return [
            lax.ppermute(a, "tm", [(i, i ^ k) for i in range(frames)])
            for k, a in enumerate(arrays, 1)
        ]

    def far(x):
        return lax.all_to_all(x, "tm", 0, 0, axis_index_groups=across, tiled=True)

    n = ROWS // NEAR
    m = n // nb
    q, k, v, g = (x.reshape(t, width) for x in (query_pre, key_pre, value_pre, grad_out))
    pair = ((2, t, WC), BF)
    share = ((n, LN), F32)
    small = ((16, LN), F32)
    state = ((ROWS, LN), F32)

    keep_kv, send_kv = call(spread_kv_kernel, [pair, pair], k, v, us=3)
    recv_kv = over(send_kv)
    own_b, ksum, *out = call(
        partial_kernel, [share, small] + [((2 * n + 32, LN), BF)] * 3, keep_kv, recv_kv, scratch=[state], us=3
    )
    got_a = near(out)
    keep_qg, send_qg, taps = call(
        spread_qg_kernel, [pair, pair, ((3, 3, WC), F32)], q, g, conv_taps, ksum, us=3
    )
    recv_qg = over(send_qg)
    local, gc_mine, gc_other, taps_part = call(
        conv_kernel,
        [((2 * t, WC), F32), ((t, WC), F32), ((t, WC), F32), ((LN, LN), F32)],
        keep_kv, recv_kv, keep_qg, recv_qg, taps, us=6,
    )
    gc_other = over(gc_other)
    pay, kpre = call(block_kernel, [((nb, 2 * m + 32, LN), BF), small], own_b, ksum, *got_a)
    got = far(pay)
    down, kt, own_d, *out = call(
        turn_kernel,
        [((nb, 2 * m, LN), BF), small, share] + [((n, LN), BF)] * 3,
        got, kpre, keep_qg, recv_qg, scratch=[state], us=4,
    )
    got_c = near(out)
    (pay,) = call(back_block_kernel, [((nb, 3 * m + 32, LN), BF)], own_d, *got_c, down, taps_part)
    got = far(pay)
    s_own, e1, e2, e3, taps_own, back = call(
        prefix_kernel,
        [share] + [((2 * n + 16, LN), BF)] * 3 + [((4, LN), F32), ((nb, m, LN), BF)],
        got, own_b, *got_a, scratch=[((NEAR, 4, LN), F32)],
    )
    got_e = near((e1, e2, e3))
    mine, other, pay, gks = call(
        attend_kernel,
        [pair, pair, ((nb, m + 48, LN), BF), small],
        *got_e, s_own, kt, keep_qg, recv_qg, local, taps_own, back, scratch=[state, small], us=4,
    )
    got = far(pay)
    whole = ((t, width), BF)
    attended, query_grad = call(merge_kernel, [whole, whole], mine, over(other), us=3)
    g0, *out = call(suffix_kernel, [((n + 32 + 8 * nb, LN), BF)] * 4, got, own_d, *got_c, gks)
    gs = [g0] + near(out)
    key_grad, value_grad, taps_grad = call(
        finish_kernel,
        [whole, whole, (conv_taps.shape, F32)],
        *gs, *[over(x) for x in gs], keep_kv, send_kv, gc_mine, gc_other,
        scratch=[state] + [((nb, NEAR, 4, LN), F32)] * 2, us=5,
    )
    return (
        attended.reshape(shape),
        query_grad.reshape(shape),
        key_grad.reshape(shape),
        value_grad.reshape(shape),
        taps_grad,
    )


def solution(mesh):
    frame = P(("groups", "tm"), "space", None, None)
    return jax.shard_map(
        shards,
        mesh=mesh,
        in_specs=(frame, frame, frame, frame, P()),
        out_specs=(frame, frame, frame, frame, P("groups", None, None)),
        check_vma=False,
    )
```

```python
import functools

import jax
import jax.numpy as jnp
from jax import lax
from jax.experimental import pallas as pl
from jax.experimental.pallas import tpu as pltpu
from jax.sharding import PartitionSpec as P

HEADS = 20
HD = 112
LN = 128
HC = 10
WC = HC * LN
NEAR = 4
ROWS = 1024
F32 = jnp.float32
BF = jnp.bfloat16
INTERPRET = False
VMEM_LIMIT = 16 << 20


def call(kernel, outs, *args, scratch=(), us=1, space=pltpu.VMEM):
    return pl.pallas_call(
        kernel,
        out_shape=[jax.ShapeDtypeStruct(s, d) for s, d in outs],
        in_specs=[pl.BlockSpec(memory_space=space)] * len(args),
        out_specs=[pl.BlockSpec(memory_space=pltpu.VMEM)] * len(outs),
        scratch_shapes=[pltpu.VMEM(*s) if isinstance(s, tuple) else s for s in scratch],
        interpret=INTERPRET,
        cost_estimate=pl.CostEstimate(flops=us * 6 * 10**9, bytes_accessed=10**6, transcendentals=0),
        compiler_params=pltpu.CompilerParams(vmem_limit_bytes=VMEM_LIMIT),
    )(*args)


def place():
    frame = lax.axis_index("tm")
    return lax.axis_index("space"), lax.rem(frame, NEAR), lax.div(frame, NEAR)


def lane(shape):
    return lax.broadcasted_iota(jnp.int32, shape, len(shape) - 1)


def halves(x):
    hi = x.astype(BF)
    return hi, (x - hi.astype(F32)).astype(BF)


def joined(hi, lo):
    return hi.astype(F32) + lo.astype(F32)


def mm(a, b, dims):
    return lax.dot_general(a, b, (dims, ((), ())), preferred_element_type=F32)


NN = ((1,), (0,))
NT = ((1,), (1,))
TN = ((0,), (0,))


def flag(cond):
    return jnp.where(cond, 1.0, 0.0).astype(F32)


def pack(ref, mats):
    last = mats[7]
    lanes = lane((HD, LN))
    for i in range(7):
        piece = pltpu.roll(last, HD - 16 * i, 1) if i < 7 else last
        ref[HD * i : HD * (i + 1), :] = jnp.where(lanes < HD, mats[i], piece)
    ref[HD * 7 : HD * 8, :] = mats[8]
    ref[HD * 8 : HD * 9, :] = mats[9]
    ref[HD * 9 : ROWS, :] = jnp.zeros((ROWS - HD * 9, LN), F32)


def unpack(ref):
    lanes = lane((HD, LN))
    mats, last = [], jnp.zeros((HD, LN), F32)
    for i in range(7):
        x = ref[HD * i : HD * (i + 1), :]
        mats.append(jnp.where(lanes < HD, x, 0.0))
        inside = (lanes >= 16 * i) & (lanes < 16 * i + 16)
        last = jnp.where(inside, pltpu.roll(x, 16 + 16 * i, 1), last)
    return mats + [last, ref[HD * 7 : HD * 8, :], ref[HD * 8 : HD * 9, :]]


def pad_rows(x):
    return jnp.concatenate([x, jnp.zeros((LN - HD, LN), x.dtype)], axis=0)


def heads_of(tile):
    out = []
    for h in range(HEADS):
        t, off = divmod(HD * h, LN)
        x = tile(t)
        if off:
            x = pltpu.roll(x, LN - off, 1)
        if off + HD > LN:
            y = pltpu.roll(tile(t + 1), LN - off, 1)
            x = jnp.where(lane(x.shape) < LN - off, x, y)
        out.append(jnp.where(lane(x.shape) < HD, x, 0.0))
    return out


def tiles_of(heads):
    out = []
    for t in range(-(-HEADS * HD // LN)):
        first, off = divmod(LN * t, HD)
        x = heads[first]
        if off:
            x = pltpu.roll(x, LN - off, 1)
        left = HD - off
        while left < LN and first + 1 < HEADS:
            first += 1
            y = pltpu.roll(heads[first], left, 1)
            x = jnp.where(lane(x.shape) < left, x, y)
            left += HD
        out.append(x)
    return out


def loader(ref, rows, width):
    cache = {}

    def tile(t):
        if t not in cache:
            n = min(LN, width - LN * t)
            x = ref[0:rows, LN * t : LN * t + n].astype(F32)
            if n < LN:
                x = jnp.concatenate([x, jnp.zeros((rows, LN - n), F32)], axis=1)
            cache[t] = x
        return cache[t]

    return tile


def spread(refs, relu, keep, send):
    first = place()[0] == 0
    for j, ref in enumerate(refs):
        rows, width = ref.shape
        heads = heads_of(loader(ref, rows, width))
        for i in range(HC):
            a, b = heads[i], heads[i + HC]
            if relu[j]:
                a, b = jnp.maximum(a, 0.0), jnp.maximum(b, 0.0)
            keep[j, :, col(i)] = lax.select(first, a, b).astype(BF)
            send[j, :, col(i)] = lax.select(first, b, a).astype(BF)


def spread_kv_kernel(k, v, keep, send, buf, sems):
    copies = [pltpu.make_async_copy(x, buf.at[j], sems.at[j]) for j, x in enumerate((k, v))]
    for c in copies:
        c.start()
    for j, c in enumerate(copies):
        c.wait()
        spread((buf.at[j],), (j == 0,), keep.at[j : j + 1], send.at[j : j + 1])


def spread_qg_kernel(q, g, taps, after, keep, send, taps_out):
    first = place()[0] == 0
    spread((q, g), (True, False), keep, send)
    for a in range(3):
        heads = heads_of(loader(taps.at[a], 3, taps.shape[2]))
        for i in range(HC):
            taps_out[a, :, col(i)] = lax.select(first, heads[i], heads[i + HC])


def col(i):
    return slice(LN * i, LN * (i + 1))


def both(keep, recv, j, i):
    return jnp.concatenate([keep[j, :, col(i)], recv[j, :, col(i)]], axis=0)


def conv_kernel(keep_v, recv_v, keep_g, recv_g, taps, local, gc_mine, gc_other, taps_out):
    first = place()[0] == 0
    half = keep_v.shape[1]
    n = 2 * half
    cols = 32
    taps_out[...] = jnp.zeros_like(taps_out)
    pos = lax.broadcasted_iota(jnp.int32, (n, LN), 0) % cols
    zero_row = jnp.zeros((cols, LN), F32)

    def shifts(keep, recv, i):
        a, b = keep[1, :, col(i)].astype(F32), recv[1, :, col(i)].astype(F32)
        x = jnp.concatenate([lax.select(first, a, b), lax.select(first, b, a)], axis=0)
        before = jnp.where(pos == 0, 0.0, pltpu.roll(x, 1, 0))
        after = jnp.where(pos == cols - 1, 0.0, pltpu.roll(x, n - 1, 0))
        return before, x, after

    def up(u):
        return jnp.concatenate([zero_row, u[: n - cols]], axis=0)

    def down(u):
        return jnp.concatenate([u[cols:], zero_row], axis=0)

    def put(mine, other, x, i):
        mine[:, col(i)] = lax.select(first, x[:half], x[half:])
        other[:, col(i)] = lax.select(first, x[half:], x[:half])

    for i in range(HC):
        w = [taps[a, :, col(i)] for a in range(3)]
        vs, gs = shifts(keep_v, recv_v, i), shifts(keep_g, recv_g, i)
        u = [sum(w[a][b : b + 1] * vs[b] for b in range(3)) for a in range(3)]
        put(local.at[0:half], local.at[half:n], up(u[0]) + u[1] + down(u[2]), i)
        u = [sum(w[a][b : b + 1] * gs[2 - b] for b in range(3)) for a in range(3)]
        put(gc_mine, gc_other, down(u[0]) + u[1] + up(u[2]), i)
        g = gs[1]
        for b in range(3):
            s = vs[b]
            for a, prod in enumerate((g[cols:] * s[: n - cols], g * s, g[: n - cols] * s[cols:])):
                r = 9 * i + 3 * a + b
                taps_out[r : r + 1, :] = jnp.sum(prod, axis=0, keepdims=True)


def rows_at(p, k, n):
    return pl.ds(pl.multiple_of((p ^ k) * n, n), n)


def put_rows(ref, *arrays):
    at = 0
    for x in arrays:
        ref[at : at + x.shape[0], :] = x
        at += x.shape[0]
    if at < ref.shape[0]:
        ref[at:, :] = jnp.zeros((ref.shape[0] - at, LN), F32)


def split(x):
    hi = x.astype(BF).astype(F32)
    return hi, x - hi


def vectors(block):
    x = block.astype(F32)
    return x[0:HC] + x[HC : 2 * HC], x[2 * HC : 3 * HC]


def partial_kernel(keep, recv, own, ksum, mean, a1, a2, a3, state, rows):
    p = place()[1]
    mats, sums, means = [], [], []
    for i in range(HC):
        keys, v = both(keep, recv, 0, i), both(keep, recv, 1, i).astype(F32)
        mid = (jnp.sum(v, axis=0, keepdims=True) * (1.0 / v.shape[0])).astype(BF).astype(F32)
        hi, lo = halves(v - mid)
        x = mm(keys, jnp.concatenate([hi, lo], axis=1), TN)[:HD]
        mats.append(x[:, :LN] + x[:, LN:])
        sums.append(jnp.sum(keys.astype(F32), axis=0, keepdims=True))
        means.append(mid)
    pack(state, mats)
    n = ROWS // NEAR
    own[...] = state[rows_at(p, 0, n), :]
    put_rows(ksum, *sums)
    put_rows(mean, *means)
    put_rows(rows, *split(ksum[0:HC, :]), mean[0:HC, :])
    block = rows[...].astype(BF)
    for k, ref in enumerate((a1, a2, a3), 1):
        ref[0:n, :] = state[rows_at(p, k, n), :].astype(BF)
        ref[n:, :] = block


def products(sums, means, i):
    free = jnp.zeros((-len(sums) % 8, LN), F32)
    a = jnp.concatenate([x[i : i + 1] for x in sums] + [free], axis=0)
    b = jnp.concatenate([x[i : i + 1] for x in means] + [free], axis=0)
    return lax.dot_general(
        a, b, (TN, ((), ())), precision=lax.Precision.HIGHEST, preferred_element_type=F32
    )[:HD]


def block_kernel(own, ksum, mean, a1, a2, a3, pay, kpre, state, rows):
    p = place()[1]
    n = ROWS // NEAR
    total, kp = own[...], ksum[0:HC, :]
    sums, means = [ksum[0:HC, :]], [mean[0:HC, :]]
    for k, ref in enumerate((a1, a2, a3), 1):
        total = total + ref[0:n, :].astype(F32)
        ks, mid = vectors(ref[n:, :])
        sums.append(ks)
        means.append(mid)
        kp = kp + flag((p ^ k) <= p) * ks
    kpre[...] = kp
    mid = (sum(means) * (1.0 / NEAR)).astype(BF).astype(F32)
    pack(state, [products(sums, [x - mid for x in means], i) for i in range(HC)])
    total = total + state[rows_at(p, 0, n), :]
    put_rows(rows, *split(sum(sums)), mid)
    block = rows[...].astype(BF)
    m = n // pay.shape[0]
    for b in range(pay.shape[0]):
        pay[b, 0:m, :] = total[m * b : m * (b + 1)].astype(BF)
        pay[b, m:, :] = block


def rank_kernel(got, ksum, mean, a1, a2, a3, rank):
    _, p, mine = place()
    n = ROWS // NEAR
    m = n // got.shape[0]
    sums, means = [ksum[0:HC, :]], [mean[0:HC, :]]
    for k, ref in enumerate((a1, a2, a3), 1):
        ks, mid = vectors(ref[n:, :])
        sums.append(flag((p ^ k) <= p) * ks)
        means.append(mid)
    for b in range(got.shape[0]):
        ks, mid = vectors(got[b, m:, :])
        sums.append(flag(b < mine) * ks)
        means.append(mid)
    for i in range(HC):
        rank[HD * i : HD * (i + 1), :] = products(sums, means, i)


def reciprocal_of(q, kt, i):
    row = jnp.broadcast_to(kt[i : i + 1, :], (LN, LN))
    hi, lo = halves(row)
    den = mm(jnp.concatenate([q, q], axis=1), jnp.concatenate([hi, lo], axis=1), NT)
    return 1.0 / (den + 1.0)


def turn_kernel(got, kpre, keep, recv, down, kt, own, c1, c2, c3, state):
    _, p, mine = place()
    nb = got.shape[0]
    n = ROWS // NEAR
    m = n // nb
    run, key_total = jnp.zeros((m, LN), F32), kpre[...]
    for b in range(nb):
        down[b] = run.astype(BF)
        run = run + got[b, 0:m, :].astype(F32)
        ks, _ = vectors(got[b, m:, :])
        key_total = key_total + flag(b < mine) * ks
    kt[...] = key_total
    mats = []
    for i in range(HC):
        q = both(keep, recv, 0, i)
        scaled = both(keep, recv, 1, i).astype(F32) * reciprocal_of(q, key_total, i)
        hi, lo = halves(scaled)
        x = mm(q, jnp.concatenate([hi, lo], axis=1), TN)[:HD]
        mats.append(x[:, :LN] + x[:, LN:])
    pack(state, mats)
    own[...] = state[rows_at(p, 0, n), :]
    for k, ref in enumerate((c1, c2, c3), 1):
        ref[...] = state[rows_at(p, k, n), :].astype(BF)


def back_block_kernel(own, c1, c2, c3, down, taps, pay, rows):
    nb = pay.shape[0]
    m = ROWS // NEAR // nb
    total = own[...]
    for ref in (c1, c2, c3):
        total = total + ref[...].astype(F32)
    for b in range(nb):
        pay[b, 0:m, :] = down[b]
        pay[b, m : 2 * m, :] = total[m * b : m * (b + 1)].astype(BF)
        put_rows(rows, *split(taps[12 * b : 12 * (b + 1), :]))
        pay[b, 2 * m :, :] = rows[...].astype(BF)


def prefix_kernel(got, own, a1, a2, a3, s_own, e1, e2, e3, taps_own, back, taps, rows):
    p = place()[1]
    nb = got.shape[0]
    n = ROWS // NEAR
    m = n // nb
    base = jnp.concatenate([got[b, 0:m, :].astype(F32) for b in range(nb)], axis=0)
    run = jnp.zeros((m, LN), F32)
    t = jnp.zeros((12, LN), F32)
    for b in reversed(range(nb)):
        back[b] = run.astype(BF)
        run = run + got[b, m : 2 * m, :].astype(F32)
        x = got[b, 2 * m :, :].astype(F32)
        t = t + (x[0:12] + x[12:24])
    for j in range(NEAR):
        taps[j] = t[3 * j : 3 * (j + 1)]
    parts = [own[...]] + [r[0:n, :].astype(F32) for r in (a1, a2, a3)]
    for k, ref in enumerate((s_own, e1, e2, e3)):
        x = base
        for j in range(NEAR):
            x = x + flag((p ^ j) <= (p ^ k)) * parts[j]
        if k == 0:
            ref[...] = x
        else:
            ref[0:n, :] = x.astype(BF)
            put_rows(rows, *split(taps[p ^ k]))
            ref[n:, :] = rows[...].astype(BF)
    taps_own[...] = taps[p]


def attend_kernel(
    e1, e2, e3, s_own, rank, kt, keep, recv, local, taps_own, back, mine, other, pay, gks, state, rows
):
    p = place()[1]
    nb = pay.shape[0]
    n = ROWS // NEAR
    m = n // nb
    half = keep.shape[1]
    state[rows_at(p, 0, n), :] = s_own[...]
    taps = taps_own[...]
    for k, ref in enumerate((e1, e2, e3), 1):
        state[rows_at(p, k, n), :] = ref[0:n, :].astype(F32)
        x = ref[n:, :].astype(F32)
        taps = taps + (x[0:3] + x[3:6])
    mats = unpack(state)
    key_total = kt[...]
    ones = jnp.ones((2 * LN, LN), BF)
    for i in range(HC):
        q, g = both(keep, recv, 0, i), both(keep, recv, 1, i)
        hi, lo = halves(pad_rows(mats[i] + rank[HD * i : HD * (i + 1), :]))
        recip = reciprocal_of(q, key_total, i)
        out = mm(jnp.concatenate([q, q], axis=1), jnp.concatenate([hi, lo], axis=0), NN) * recip
        x = (out + local[:, col(i)]).astype(BF)
        mine[0, :, col(i)] = x[:half]
        other[0, :, col(i)] = x[half:]
        ghi, glo = halves(g.astype(F32) * out)
        gden = -mm(jnp.concatenate([ghi, glo], axis=1), ones, NN) * recip
        gs = mm(jnp.concatenate([g, g], axis=1), jnp.concatenate([hi, lo], axis=1), NT)
        qf = q.astype(F32)
        x = jnp.where(qf > 0.0, gs * recip + gden * key_total[i : i + 1, :], 0.0).astype(BF)
        mine[1, :, col(i)] = x[:half]
        other[1, :, col(i)] = x[half:]
        gks[i : i + 1, :] = jnp.sum(gden * qf, axis=0, keepdims=True)
    put_rows(rows, *split(gks[...]), *split(taps))
    block = rows[...].astype(BF)
    for b in range(nb):
        pay[b, 0:m, :] = back[b]
        pay[b, m:, :] = block


def suffix_kernel(got, own, c1, c2, c3, gks, g0, g1, g2, g3, rows):
    _, p, mine = place()
    nb = got.shape[0]
    n = ROWS // NEAR
    m = n // nb
    base = jnp.concatenate([got[b, 0:m, :].astype(F32) for b in range(nb)], axis=0)
    later = jnp.zeros((HC, LN), F32)
    taps = []
    for b in range(nb):
        x = got[b, m:, :].astype(F32)
        later = later + flag(b > mine) * (x[0:HC] + x[HC : 2 * HC])
        taps.append(x[2 * HC : 2 * HC + 3] + x[2 * HC + 3 : 2 * HC + 6])
    his, los = zip(*(split(x) for x in taps))
    parts = [own[...]] + [r[...].astype(F32) for r in (c1, c2, c3)]
    for k, ref in enumerate((g0, g1, g2, g3)):
        x = base
        for j in range(NEAR):
            x = x + flag((p ^ j) >= (p ^ k)) * parts[j]
        ref[0:n, :] = x.astype(BF)
        put_rows(rows, *split(later + flag(p >= (p ^ k)) * gks[...]), *his, *los)
        ref[n:, :] = rows[...].astype(BF)


def assembled(refs, state, taps):
    p = place()[1]
    n = ROWS // NEAR
    nb = taps.shape[0]
    total = jnp.zeros((HC, LN), F32)
    for k, ref in enumerate(refs):
        state[rows_at(p, k, n), :] = ref[0:n, :].astype(F32)
        x = ref[n:, :].astype(F32)
        total = total + (x[0:HC] + x[HC : 2 * HC])
        for b in range(nb):
            at = 2 * HC + 3 * b
            taps[b, p ^ k] = x[at : at + 3] + x[at + 3 * nb : at + 3 * nb + 3]
    return unpack(state), total


def finish_kernel(
    g0, g1, g2, g3, o0, o1, o2, o3, keep, send, gc_mine, gc_other, key, value, taps, state, taps_a, taps_b
):
    first = place()[0] == 0
    sides = []
    for refs, tokens, conv, scratch in (
        ((g0, g1, g2, g3), keep, gc_mine, taps_a),
        ((o0, o1, o2, o3), send, gc_other, taps_b),
    ):
        mats, total = assembled(refs, state, scratch)
        keys_out, values_out, taps_out = [], [], []
        for i in range(HC):
            keys, v = tokens[0, :, col(i)], tokens[1, :, col(i)]
            hi, lo = halves(pad_rows(mats[i]))
            gk = mm(jnp.concatenate([v, v], axis=1), jnp.concatenate([hi, lo], axis=1), NT)
            keys_out.append(jnp.where(keys.astype(F32) > 0.0, gk + total[i : i + 1, :], 0.0))
            gm = mm(jnp.concatenate([keys, keys], axis=1), jnp.concatenate([hi, lo], axis=0), NN)
            values_out.append(gm + conv[:, col(i)])
        sides.append((keys_out, values_out))
    for j, ref in enumerate((key, value)):
        gather_heads(first, sides[0][j], sides[1][j], ref)
    for a in range(3):
        rows = []
        for scratch in (taps_a, taps_b):
            heads = []
            for i in range(HC):
                lines = []
                for b in range(3):
                    r = 9 * i + 3 * a + b
                    lines.append(scratch[r // 12, (r % 12) // 3, r % 3 : r % 3 + 1, :])
                heads.append(jnp.concatenate(lines, axis=0))
            rows.append(heads)
        gather_heads(first, rows[0], rows[1], taps.at[a])


def gather_heads(first, mine, other, ref):
    heads = [lax.select(first, mine[i], other[i]) for i in range(HC)]
    heads += [lax.select(first, other[i], mine[i]) for i in range(HC)]
    width = ref.shape[1]
    for t, x in enumerate(tiles_of(heads)):
        n = min(LN, width - LN * t)
        ref[:, LN * t : LN * t + n] = x[:, :n].astype(ref.dtype)


def merge_kernel(mine, other, out_a, out_b):
    first = place()[0] == 0
    for j, ref in enumerate((out_a, out_b)):
        heads = [[x[j, :, col(i)].astype(F32) for i in range(HC)] for x in (mine, other)]
        gather_heads(first, heads[0], heads[1], ref)


def shards(query_pre, key_pre, value_pre, grad_out, conv_taps):
    shape = value_pre.shape
    width = shape[-1]
    t = shape[0] * shape[1] * shape[2]
    frames = lax.axis_size("tm")
    nb = frames // NEAR
    across = [[j + NEAR * b for b in range(nb)] for j in range(NEAR)]

    def over(x):
        return lax.ppermute(x, "space", [(0, 1), (1, 0)])

    def near(arrays):
        return [
            lax.ppermute(a, "tm", [(i, i ^ k) for i in range(frames)])
            for k, a in enumerate(arrays, 1)
        ]

    def far(x):
        return lax.all_to_all(x, "tm", 0, 0, axis_index_groups=across, tiled=True)

    n = ROWS // NEAR
    m = n // nb
    q, k, v, g = (x.reshape(t, width) for x in (query_pre, key_pre, value_pre, grad_out))
    pair = ((2, t, WC), BF)
    share = ((n, LN), F32)
    small = ((16, LN), F32)
    row = ((HC, LN), F32)
    state = ((ROWS, LN), F32)

    keep_kv, send_kv = call(
        spread_kv_kernel,
        [pair, pair],
        k, v, us=1, space=pltpu.HBM,
        scratch=[((2, t, width), BF), pltpu.SemaphoreType.DMA((2,))],
    )
    recv_kv = over(send_kv)
    own_b, ksum, mean, *out = call(
        partial_kernel,
        [share, small, small] + [((n + 32, LN), BF)] * 3,
        keep_kv, recv_kv, scratch=[state, ((32, LN), F32)], us=1,
    )
    got_a = near(out)
    keep_qg, send_qg, taps = call(
        spread_qg_kernel, [pair, pair, ((3, 3, WC), F32)], q, g, conv_taps, ksum, us=3
    )
    recv_qg = over(send_qg)
    local, gc_mine, gc_other, taps_part = call(
        conv_kernel,
        [((2 * t, WC), F32), ((t, WC), F32), ((t, WC), F32), ((96, LN), F32)],
        keep_kv, recv_kv, keep_qg, recv_qg, taps, us=6,
    )
    gc_other = over(gc_other)
    pay, kpre = call(
        block_kernel,
        [((nb, m + 32, LN), BF), row],
        own_b, ksum, mean, *got_a, scratch=[state, ((32, LN), F32)],
    )
    got = far(pay)
    down, kt, own_d, *out = call(
        turn_kernel,
        [((nb, m, LN), BF), row, share] + [((n, LN), BF)] * 3,
        got, kpre, keep_qg, recv_qg, scratch=[state], us=4,
    )
    got_c = near(out)
    (pay,) = call(
        back_block_kernel,
        [((nb, 2 * m + 24, LN), BF)],
        own_d, *got_c, down, taps_part, scratch=[((24, LN), F32)],
    )
    (rank,) = call(rank_kernel, [((HC * HD, LN), F32)], got, ksum, mean, *got_a, us=2)
    got = far(pay)
    s_own, e1, e2, e3, taps_own, back = call(
        prefix_kernel,
        [share] + [((n + 16, LN), BF)] * 3 + [((3, LN), F32), ((nb, m, LN), BF)],
        got, own_b, *got_a, scratch=[((NEAR, 3, LN), F32), ((16, LN), F32)],
    )
    got_e = near((e1, e2, e3))
    mine, other, pay, gks = call(
        attend_kernel,
        [pair, pair, ((nb, m + 32, LN), BF), row],
        *got_e, s_own, rank, kt, keep_qg, recv_qg, local, taps_own, back,
        scratch=[state, ((32, LN), F32)], us=4,
    )
    got = far(pay)
    whole = ((t, width), BF)
    attended, query_grad = call(merge_kernel, [whole, whole], mine, over(other), us=3)
    tail = -(-(2 * HC + 6 * nb) // 8) * 8
    g0, *out = call(
        suffix_kernel,
        [((n + tail, LN), BF)] * 4,
        got, own_d, *got_c, gks, scratch=[((tail, LN), F32)],
    )
    gs = [g0] + near(out)
    key_grad, value_grad, taps_grad = call(
        finish_kernel,
        [whole, whole, (conv_taps.shape, F32)],
        *gs, *[over(x) for x in gs], keep_kv, send_kv, gc_mine, gc_other,
        scratch=[state] + [((nb, NEAR, 3, LN), F32)] * 2, us=5,
    )
    return (
        attended.reshape(shape),
        query_grad.reshape(shape),
        key_grad.reshape(shape),
        value_grad.reshape(shape),
        taps_grad,
    )


def solution(mesh):
    frame = P(("groups", "tm"), "space", None, None)
    return jax.shard_map(
        shards,
        mesh=mesh,
        in_specs=(frame, frame, frame, frame, P()),
        out_specs=(frame, frame, frame, frame, P("groups", None, None)),
        check_vma=False,
    )
```

```python
import functools

import jax
import jax.numpy as jnp
from jax import lax
from jax.experimental import pallas as pl
from jax.experimental.pallas import tpu as pltpu
from jax.sharding import PartitionSpec as P

HEADS = 20
HD = 112
LN = 128
HC = 10
WC = HC * LN
NEAR = 4
ROWS = 1024
F32 = jnp.float32
BF = jnp.bfloat16
INTERPRET = False
VMEM_LIMIT = 16 << 20


def call(kernel, outs, *args, scratch=(), us=1):
    return pl.pallas_call(
        kernel,
        out_shape=[jax.ShapeDtypeStruct(s, d) for s, d in outs],
        in_specs=[pl.BlockSpec(memory_space=pltpu.VMEM)] * len(args),
        out_specs=[pl.BlockSpec(memory_space=pltpu.VMEM)] * len(outs),
        scratch_shapes=[pltpu.VMEM(*s) if isinstance(s, tuple) else s for s in scratch],
        interpret=INTERPRET,
        cost_estimate=pl.CostEstimate(flops=us * 10**10, bytes_accessed=10**6, transcendentals=0),
        compiler_params=pltpu.CompilerParams(vmem_limit_bytes=VMEM_LIMIT),
    )(*args)


def place():
    frame = lax.axis_index("tm")
    return lax.axis_index("space"), lax.rem(frame, NEAR), lax.div(frame, NEAR)


def lane(shape):
    return lax.broadcasted_iota(jnp.int32, shape, len(shape) - 1)


def halves(x):
    hi = x.astype(BF)
    return hi, (x - hi.astype(F32)).astype(BF)


def joined(hi, lo):
    return hi.astype(F32) + lo.astype(F32)


def mm(a, b, dims):
    return lax.dot_general(a, b, (dims, ((), ())), preferred_element_type=F32)


NN = ((1,), (0,))
NT = ((1,), (1,))
TN = ((0,), (0,))


def flag(cond):
    return jnp.where(cond, 1.0, 0.0).astype(F32)


def pack(ref, mats):
    last = mats[7]
    lanes = lane((HD, LN))
    for i in range(7):
        piece = pltpu.roll(last, HD - 16 * i, 1) if i < 7 else last
        ref[HD * i : HD * (i + 1), :] = jnp.where(lanes < HD, mats[i], piece)
    ref[HD * 7 : HD * 8, :] = mats[8]
    ref[HD * 8 : HD * 9, :] = mats[9]
    ref[HD * 9 : ROWS, :] = jnp.zeros((ROWS - HD * 9, LN), F32)


def unpack(ref):
    lanes = lane((HD, LN))
    mats, last = [], jnp.zeros((HD, LN), F32)
    for i in range(7):
        x = ref[HD * i : HD * (i + 1), :]
        mats.append(jnp.where(lanes < HD, x, 0.0))
        inside = (lanes >= 16 * i) & (lanes < 16 * i + 16)
        last = jnp.where(inside, pltpu.roll(x, 16 + 16 * i, 1), last)
    return mats + [last, ref[HD * 7 : HD * 8, :], ref[HD * 8 : HD * 9, :]]


def pad_rows(x):
    return jnp.concatenate([x, jnp.zeros((LN - HD, LN), x.dtype)], axis=0)


def heads_of(tile):
    out = []
    for h in range(HEADS):
        t, off = divmod(HD * h, LN)
        x = tile(t)
        if off:
            x = pltpu.roll(x, LN - off, 1)
        if off + HD > LN:
            y = pltpu.roll(tile(t + 1), LN - off, 1)
            x = jnp.where(lane(x.shape) < LN - off, x, y)
        out.append(jnp.where(lane(x.shape) < HD, x, 0.0))
    return out


def tiles_of(heads):
    out = []
    for t in range(-(-HEADS * HD // LN)):
        first, off = divmod(LN * t, HD)
        x = heads[first]
        if off:
            x = pltpu.roll(x, LN - off, 1)
        left = HD - off
        while left < LN and first + 1 < HEADS:
            first += 1
            y = pltpu.roll(heads[first], left, 1)
            x = jnp.where(lane(x.shape) < left, x, y)
            left += HD
        out.append(x)
    return out


def loader(ref, rows, width):
    cache = {}

    def tile(t):
        if t not in cache:
            n = min(LN, width - LN * t)
            x = ref[0:rows, LN * t : LN * t + n].astype(F32)
            if n < LN:
                x = jnp.concatenate([x, jnp.zeros((rows, LN - n), F32)], axis=1)
            cache[t] = x
        return cache[t]

    return tile


def spread(refs, relu, keep, send):
    first = place()[0] == 0
    for j, ref in enumerate(refs):
        rows, width = ref.shape
        heads = heads_of(loader(ref, rows, width))
        for i in range(HC):
            a, b = heads[i], heads[i + HC]
            if relu[j]:
                a, b = jnp.maximum(a, 0.0), jnp.maximum(b, 0.0)
            keep[j, :, col(i)] = lax.select(first, a, b).astype(BF)
            send[j, :, col(i)] = lax.select(first, b, a).astype(BF)


def spread_k_kernel(k, keep, send):
    spread((k,), (True,), keep, send)


def spread_v_kernel(v, keep, send):
    spread((v,), (False,), keep, send)


def spread_qg_kernel(q, g, taps, after, keep, send, taps_out):
    first = place()[0] == 0
    spread((q, g), (True, False), keep, send)
    for a in range(3):
        heads = heads_of(loader(taps.at[a], 3, taps.shape[2]))
        for i in range(HC):
            taps_out[a, :, col(i)] = lax.select(first, heads[i], heads[i + HC])


def col(i):
    return slice(LN * i, LN * (i + 1))


def both(keep, recv, j, i):
    return jnp.concatenate([keep[j, :, col(i)], recv[j, :, col(i)]], axis=0)


def conv_kernel(keep_v, recv_v, keep_g, recv_g, taps, local, gc_mine, gc_other, taps_out):
    first = place()[0] == 0
    half = keep_v.shape[1]
    n = 2 * half
    cols = 32
    taps_out[...] = jnp.zeros_like(taps_out)
    pos = lax.broadcasted_iota(jnp.int32, (n, LN), 0) % cols
    zero_row = jnp.zeros((cols, LN), F32)

    def shifts(keep, recv, j, i):
        a, b = keep[j, :, col(i)].astype(F32), recv[j, :, col(i)].astype(F32)
        x = jnp.concatenate([lax.select(first, a, b), lax.select(first, b, a)], axis=0)
        before = jnp.where(pos == 0, 0.0, pltpu.roll(x, 1, 0))
        after = jnp.where(pos == cols - 1, 0.0, pltpu.roll(x, n - 1, 0))
        return before, x, after

    def up(u):
        return jnp.concatenate([zero_row, u[: n - cols]], axis=0)

    def down(u):
        return jnp.concatenate([u[cols:], zero_row], axis=0)

    def put(mine, other, x, i):
        mine[:, col(i)] = lax.select(first, x[:half], x[half:])
        other[:, col(i)] = lax.select(first, x[half:], x[:half])

    for i in range(HC):
        w = [taps[a, :, col(i)] for a in range(3)]
        vs, gs = shifts(keep_v, recv_v, 0, i), shifts(keep_g, recv_g, 1, i)
        u = [sum(w[a][b : b + 1] * vs[b] for b in range(3)) for a in range(3)]
        put(local.at[0:half], local.at[half:n], up(u[0]) + u[1] + down(u[2]), i)
        u = [sum(w[a][b : b + 1] * gs[2 - b] for b in range(3)) for a in range(3)]
        put(gc_mine, gc_other, down(u[0]) + u[1] + up(u[2]), i)
        g = gs[1]
        for b in range(3):
            s = vs[b]
            for a, prod in enumerate((g[cols:] * s[: n - cols], g * s, g[: n - cols] * s[cols:])):
                r = 9 * i + 3 * a + b
                taps_out[r : r + 1, :] = jnp.sum(prod, axis=0, keepdims=True)


def rows_at(p, k, n):
    return pl.ds(pl.multiple_of((p ^ k) * n, n), n)


def put_rows(ref, *arrays):
    at = 0
    for x in arrays:
        ref[at : at + x.shape[0], :] = x
        at += x.shape[0]
    if at < ref.shape[0]:
        ref[at:, :] = jnp.zeros((ref.shape[0] - at, LN), F32)


def split(x):
    hi = x.astype(BF).astype(F32)
    return hi, x - hi


def vectors(block):
    x = block.astype(F32)
    return x[0:HC] + x[HC : 2 * HC], x[2 * HC : 3 * HC]


def partial_kernel(keep_k, recv_k, keep_v, recv_v, own, ksum, mean, a1, a2, a3, state, rows):
    p = place()[1]
    mats, sums, means = [], [], []
    for i in range(HC):
        keys, v = both(keep_k, recv_k, 0, i), both(keep_v, recv_v, 0, i).astype(F32)
        mid = (jnp.sum(v, axis=0, keepdims=True) * (1.0 / v.shape[0])).astype(BF).astype(F32)
        hi, lo = halves(v - mid)
        x = mm(keys, jnp.concatenate([hi, lo], axis=1), TN)[:HD]
        mats.append(x[:, :LN] + x[:, LN:])
        sums.append(jnp.sum(keys.astype(F32), axis=0, keepdims=True))
        means.append(mid)
    pack(state, mats)
    n = ROWS // NEAR
    own[...] = state[rows_at(p, 0, n), :]
    put_rows(ksum, *sums)
    put_rows(mean, *means)
    put_rows(rows, *split(ksum[0:HC, :]), mean[0:HC, :])
    block = rows[...].astype(BF)
    for k, ref in enumerate((a1, a2, a3), 1):
        ref[0:n, :] = state[rows_at(p, k, n), :].astype(BF)
        ref[n:, :] = block


def products(sums, means, i):
    free = jnp.zeros((-len(sums) % 8, LN), F32)
    a = jnp.concatenate([x[i : i + 1] for x in sums] + [free], axis=0)
    b = jnp.concatenate([x[i : i + 1] for x in means] + [free], axis=0)
    return lax.dot_general(
        a, b, (TN, ((), ())), precision=lax.Precision.HIGHEST, preferred_element_type=F32
    )[:HD]


def block_kernel(own, ksum, mean, a1, a2, a3, pay, kpre, state, rows):
    p = place()[1]
    n = ROWS // NEAR
    total, kp = own[...], ksum[0:HC, :]
    sums, means = [ksum[0:HC, :]], [mean[0:HC, :]]
    for k, ref in enumerate((a1, a2, a3), 1):
        total = total + ref[0:n, :].astype(F32)
        ks, mid = vectors(ref[n:, :])
        sums.append(ks)
        means.append(mid)
        kp = kp + flag((p ^ k) <= p) * ks
    kpre[...] = kp
    mid = (sum(means) * (1.0 / NEAR)).astype(BF).astype(F32)
    pack(state, [products(sums, [x - mid for x in means], i) for i in range(HC)])
    total = total + state[rows_at(p, 0, n), :]
    put_rows(rows, *split(sum(sums)), mid)
    block = rows[...].astype(BF)
    m = n // pay.shape[0]
    for b in range(pay.shape[0]):
        pay[b, 0:m, :] = total[m * b : m * (b + 1)].astype(BF)
        pay[b, m:, :] = block


def rank_kernel(got, ksum, mean, a1, a2, a3, rank):
    _, p, mine = place()
    n = ROWS // NEAR
    m = n // got.shape[0]
    sums, means = [ksum[0:HC, :]], [mean[0:HC, :]]
    for k, ref in enumerate((a1, a2, a3), 1):
        ks, mid = vectors(ref[n:, :])
        sums.append(flag((p ^ k) <= p) * ks)
        means.append(mid)
    for b in range(got.shape[0]):
        ks, mid = vectors(got[b, m:, :])
        sums.append(flag(b < mine) * ks)
        means.append(mid)
    for i in range(HC):
        rank[HD * i : HD * (i + 1), :] = products(sums, means, i)


def reciprocal_of(q, kt, i):
    row = jnp.broadcast_to(kt[i : i + 1, :], (LN, LN))
    hi, lo = halves(row)
    den = mm(jnp.concatenate([q, q], axis=1), jnp.concatenate([hi, lo], axis=1), NT)
    return 1.0 / (den + 1.0)


def turn_kernel(got, kpre, keep, recv, after, down, kt, own, c1, c2, c3, state):
    _, p, mine = place()
    nb = got.shape[0]
    n = ROWS // NEAR
    m = n // nb
    run, key_total = jnp.zeros((m, LN), F32), kpre[...]
    for b in range(nb):
        down[b] = run.astype(BF)
        run = run + got[b, 0:m, :].astype(F32)
        ks, _ = vectors(got[b, m:, :])
        key_total = key_total + flag(b < mine) * ks
    kt[...] = key_total
    mats = []
    for i in range(HC):
        q = both(keep, recv, 0, i)
        scaled = both(keep, recv, 1, i).astype(F32) * reciprocal_of(q, key_total, i)
        hi, lo = halves(scaled)
        x = mm(q, jnp.concatenate([hi, lo], axis=1), TN)[:HD]
        mats.append(x[:, :LN] + x[:, LN:])
    pack(state, mats)
    own[...] = state[rows_at(p, 0, n), :]
    for k, ref in enumerate((c1, c2, c3), 1):
        ref[...] = state[rows_at(p, k, n), :].astype(BF)


def back_block_kernel(own, c1, c2, c3, down, taps, pay, rows):
    nb = pay.shape[0]
    m = ROWS // NEAR // nb
    total = own[...]
    for ref in (c1, c2, c3):
        total = total + ref[...].astype(F32)
    for b in range(nb):
        pay[b, 0:m, :] = down[b]
        pay[b, m : 2 * m, :] = total[m * b : m * (b + 1)].astype(BF)
        put_rows(rows, *split(taps[12 * b : 12 * (b + 1), :]))
        pay[b, 2 * m :, :] = rows[...].astype(BF)


def prefix_kernel(got, own, a1, a2, a3, s_own, e1, e2, e3, taps_own, back, taps, rows):
    p = place()[1]
    nb = got.shape[0]
    n = ROWS // NEAR
    m = n // nb
    base = jnp.concatenate([got[b, 0:m, :].astype(F32) for b in range(nb)], axis=0)
    run = jnp.zeros((m, LN), F32)
    t = jnp.zeros((12, LN), F32)
    for b in reversed(range(nb)):
        back[b] = run.astype(BF)
        run = run + got[b, m : 2 * m, :].astype(F32)
        x = got[b, 2 * m :, :].astype(F32)
        t = t + (x[0:12] + x[12:24])
    for j in range(NEAR):
        taps[j] = t[3 * j : 3 * (j + 1)]
    parts = [own[...]] + [r[0:n, :].astype(F32) for r in (a1, a2, a3)]
    for k, ref in enumerate((s_own, e1, e2, e3)):
        x = base
        for j in range(NEAR):
            x = x + flag((p ^ j) <= (p ^ k)) * parts[j]
        if k == 0:
            ref[...] = x
        else:
            ref[0:n, :] = x.astype(BF)
            put_rows(rows, *split(taps[p ^ k]))
            ref[n:, :] = rows[...].astype(BF)
    taps_own[...] = taps[p]


def attend_kernel(
    e1, e2, e3, s_own, rank, kt, keep, recv, local, taps_own, back, mine, other, pay, gks, state, rows
):
    p = place()[1]
    nb = pay.shape[0]
    n = ROWS // NEAR
    m = n // nb
    half = keep.shape[1]
    state[rows_at(p, 0, n), :] = s_own[...]
    taps = taps_own[...]
    for k, ref in enumerate((e1, e2, e3), 1):
        state[rows_at(p, k, n), :] = ref[0:n, :].astype(F32)
        x = ref[n:, :].astype(F32)
        taps = taps + (x[0:3] + x[3:6])
    mats = unpack(state)
    key_total = kt[...]
    ones = jnp.ones((2 * LN, LN), BF)
    for i in range(HC):
        q, g = both(keep, recv, 0, i), both(keep, recv, 1, i)
        hi, lo = halves(pad_rows(mats[i] + rank[HD * i : HD * (i + 1), :]))
        recip = reciprocal_of(q, key_total, i)
        out = mm(jnp.concatenate([q, q], axis=1), jnp.concatenate([hi, lo], axis=0), NN) * recip
        x = (out + local[:, col(i)]).astype(BF)
        mine[0, :, col(i)] = x[:half]
        other[0, :, col(i)] = x[half:]
        ghi, glo = halves(g.astype(F32) * out)
        gden = -mm(jnp.concatenate([ghi, glo], axis=1), ones, NN) * recip
        gs = mm(jnp.concatenate([g, g], axis=1), jnp.concatenate([hi, lo], axis=1), NT)
        qf = q.astype(F32)
        x = jnp.where(qf > 0.0, gs * recip + gden * key_total[i : i + 1, :], 0.0).astype(BF)
        mine[1, :, col(i)] = x[:half]
        other[1, :, col(i)] = x[half:]
        gks[i : i + 1, :] = jnp.sum(gden * qf, axis=0, keepdims=True)
    put_rows(rows, gks[...], *split(taps))
    block = rows[...].astype(BF)
    for b in range(nb):
        pay[b, 0:m, :] = back[b]
        pay[b, m:, :] = block


def suffix_kernel(got, own, c1, c2, c3, gks, after, g0, g1, g2, g3, rows):
    _, p, mine = place()
    nb = got.shape[0]
    n = ROWS // NEAR
    m = n // nb
    base = jnp.concatenate([got[b, 0:m, :].astype(F32) for b in range(nb)], axis=0)
    later = jnp.zeros((HC, LN), F32)
    taps = []
    for b in range(nb):
        x = got[b, m:, :].astype(F32)
        later = later + flag(b > mine) * x[0:HC]
        taps.append(x[HC : HC + 3] + x[HC + 3 : HC + 6])
    taps = jnp.concatenate(taps, axis=0)
    parts = [own[...]] + [r[...].astype(F32) for r in (c1, c2, c3)]
    for k, ref in enumerate((g0, g1, g2, g3)):
        x = base
        for j in range(NEAR):
            x = x + flag((p ^ j) >= (p ^ k)) * parts[j]
        ref[0:n, :] = x.astype(BF)
        put_rows(rows, later + flag(p >= (p ^ k)) * gks[...], jnp.zeros((HC, LN), F32), *split(taps))
        ref[n:, :] = rows[...].astype(BF)


def assembled(refs, state, taps):
    p = place()[1]
    n = ROWS // NEAR
    nb = taps.shape[0]
    total = jnp.zeros((HC, LN), F32)
    for k, ref in enumerate(refs):
        state[rows_at(p, k, n), :] = ref[0:n, :].astype(F32)
        x = ref[n:, :].astype(F32)
        total = total + x[0:HC]
        for b in range(nb):
            at = 2 * HC + 3 * b
            taps[b, p ^ k] = x[at : at + 3] + x[at + 3 * nb : at + 3 * nb + 3]
    return unpack(state), total


def finish_kernel(
    g0, g1, g2, g3, o0, o1, o2, o3, keep_k, keep_v, send_k, send_v, gc_mine, gc_other, key, value, taps, state, taps_a, taps_b
):
    first = place()[0] == 0
    sides = []
    for refs, tokens, conv, scratch in (
        ((g0, g1, g2, g3), (keep_k, keep_v), gc_mine, taps_a),
        ((o0, o1, o2, o3), (send_k, send_v), gc_other, taps_b),
    ):
        mats, total = assembled(refs, state, scratch)
        keys_out, values_out, taps_out = [], [], []
        for i in range(HC):
            keys, v = tokens[0][0, :, col(i)], tokens[1][0, :, col(i)]
            hi, lo = halves(pad_rows(mats[i]))
            gk = mm(jnp.concatenate([v, v], axis=1), jnp.concatenate([hi, lo], axis=1), NT)
            keys_out.append(jnp.where(keys.astype(F32) > 0.0, gk + total[i : i + 1, :], 0.0))
            gm = mm(jnp.concatenate([keys, keys], axis=1), jnp.concatenate([hi, lo], axis=0), NN)
            values_out.append(gm + conv[:, col(i)])
        sides.append((keys_out, values_out))
    for j, ref in enumerate((key, value)):
        gather_heads(first, sides[0][j], sides[1][j], ref)
    for a in range(3):
        rows = []
        for scratch in (taps_a, taps_b):
            heads = []
            for i in range(HC):
                lines = []
                for b in range(3):
                    r = 9 * i + 3 * a + b
                    lines.append(scratch[r // 12, (r % 12) // 3, r % 3 : r % 3 + 1, :])
                heads.append(jnp.concatenate(lines, axis=0))
            rows.append(heads)
        gather_heads(first, rows[0], rows[1], taps.at[a])


def gather_heads(first, mine, other, ref):
    heads = [lax.select(first, mine[i], other[i]) for i in range(HC)]
    heads += [lax.select(first, other[i], mine[i]) for i in range(HC)]
    width = ref.shape[1]
    for t, x in enumerate(tiles_of(heads)):
        n = min(LN, width - LN * t)
        ref[:, LN * t : LN * t + n] = x[:, :n].astype(ref.dtype)


def merge_kernel(mine, other, out_a, out_b, done):
    done[...] = jnp.zeros_like(done)
    first = place()[0] == 0
    for j, ref in enumerate((out_a, out_b)):
        heads = [[x[j, :, col(i)].astype(F32) for i in range(HC)] for x in (mine, other)]
        gather_heads(first, heads[0], heads[1], ref)


def shards(query_pre, key_pre, value_pre, grad_out, conv_taps):
    shape = value_pre.shape
    width = shape[-1]
    t = shape[0] * shape[1] * shape[2]
    frames = lax.axis_size("tm")
    nb = frames // NEAR
    across = [[j + NEAR * b for b in range(nb)] for j in range(NEAR)]

    def over(x):
        return lax.ppermute(x, "space", [(0, 1), (1, 0)])

    def near(arrays):
        return [
            lax.ppermute(a, "tm", [(i, i ^ k) for i in range(frames)])
            for k, a in enumerate(arrays, 1)
        ]

    def far(x):
        return lax.all_to_all(x, "tm", 0, 0, axis_index_groups=across, tiled=True)

    n = ROWS // NEAR
    m = n // nb
    q, k, v, g = (x.reshape(t, width) for x in (query_pre, key_pre, value_pre, grad_out))
    pair = ((2, t, WC), BF)
    share = ((n, LN), F32)
    small = ((16, LN), F32)
    row = ((HC, LN), F32)
    state = ((ROWS, LN), F32)

    one = ((1, t, WC), BF)
    keep_k, send_k = call(spread_k_kernel, [one, one], k)
    recv_k = over(send_k)
    keep_v, send_v = call(spread_v_kernel, [one, one], v)
    recv_v = over(send_v)
    own_b, ksum, mean, *out = call(
        partial_kernel,
        [share, small, small] + [((n + 32, LN), BF)] * 3,
        keep_k, recv_k, keep_v, recv_v, scratch=[state, ((32, LN), F32)], us=1,
    )
    got_a = near(out)
    keep_qg, send_qg, taps = call(
        spread_qg_kernel, [pair, pair, ((3, 3, WC), F32)], q, g, conv_taps, ksum, us=1
    )
    recv_qg = over(send_qg)
    local, gc_mine, gc_other, taps_part = call(
        conv_kernel,
        [((2 * t, WC), F32), ((t, WC), F32), ((t, WC), F32), ((96, LN), F32)],
        keep_v, recv_v, keep_qg, recv_qg, taps, us=1,
    )
    gc_other = over(gc_other)
    pay, kpre = call(
        block_kernel,
        [((nb, m + 32, LN), BF), row],
        own_b, ksum, mean, *got_a, scratch=[state, ((32, LN), F32)],
    )
    got = far(pay)
    down, kt, own_d, *out = call(
        turn_kernel,
        [((nb, m, LN), BF), row, share] + [((n, LN), BF)] * 3,
        got, kpre, keep_qg, recv_qg, taps_part, scratch=[state], us=4,
    )
    got_c = near(out)
    (pay,) = call(
        back_block_kernel,
        [((nb, 2 * m + 24, LN), BF)],
        own_d, *got_c, down, taps_part, scratch=[((24, LN), F32)],
    )
    (rank,) = call(rank_kernel, [((HC * HD, LN), F32)], got, ksum, mean, *got_a, us=2)
    got = far(pay)
    s_own, e1, e2, e3, taps_own, back = call(
        prefix_kernel,
        [share] + [((n + 16, LN), BF)] * 3 + [((3, LN), F32), ((nb, m, LN), BF)],
        got, own_b, *got_a, scratch=[((NEAR, 3, LN), F32), ((16, LN), F32)],
    )
    got_e = near((e1, e2, e3))
    mine, other, pay, gks = call(
        attend_kernel,
        [pair, pair, ((nb, m + 16, LN), BF), row],
        *got_e, s_own, rank, kt, keep_qg, recv_qg, local, taps_own, back,
        scratch=[state, ((16, LN), F32)], us=4,
    )
    got = far(pay)
    whole = ((t, width), BF)
    attended, query_grad, done = call(
        merge_kernel, [whole, whole, ((8, LN), F32)], mine, over(other), us=2
    )
    tail = -(-(2 * HC + 6 * nb) // 8) * 8
    g0, *out = call(
        suffix_kernel,
        [((n + tail, LN), BF)] * 4,
        got, own_d, *got_c, gks, done, scratch=[((tail, LN), F32)],
    )
    gs = [g0] + near(out)
    key_grad, value_grad, taps_grad = call(
        finish_kernel,
        [whole, whole, (conv_taps.shape, F32)],
        *gs, *[over(x) for x in gs], keep_k, keep_v, send_k, send_v, gc_mine, gc_other,
        scratch=[state] + [((nb, NEAR, 3, LN), F32)] * 2, us=5,
    )
    return (
        attended.reshape(shape),
        query_grad.reshape(shape),
        key_grad.reshape(shape),
        value_grad.reshape(shape),
        taps_grad,
    )


def solution(mesh):
    frame = P(("groups", "tm"), "space", None, None)
    return jax.shard_map(
        shards,
        mesh=mesh,
        in_specs=(frame, frame, frame, frame, P()),
        out_specs=(frame, frame, frame, frame, P("groups", None, None)),
        check_vma=False,
    )
```

```python
import functools

import jax
import jax.numpy as jnp
from jax import lax
from jax.experimental import pallas as pl
from jax.experimental.pallas import tpu as pltpu
from jax.sharding import PartitionSpec as P

HEADS = 20
HD = 112
LN = 128
HC = 10
WC = HC * LN
NEAR = 4
ROWS = 1024
F32 = jnp.float32
BF = jnp.bfloat16
INTERPRET = False
VMEM_LIMIT = 16 << 20


def call(kernel, outs, *args, scratch=(), us=1):
    return pl.pallas_call(
        kernel,
        out_shape=[jax.ShapeDtypeStruct(s, d) for s, d in outs],
        in_specs=[pl.BlockSpec(memory_space=pltpu.VMEM)] * len(args),
        out_specs=[pl.BlockSpec(memory_space=pltpu.VMEM)] * len(outs),
        scratch_shapes=[pltpu.VMEM(*s) if isinstance(s, tuple) else s for s in scratch],
        interpret=INTERPRET,
        cost_estimate=pl.CostEstimate(flops=us * 10**10, bytes_accessed=10**6, transcendentals=0),
        compiler_params=pltpu.CompilerParams(vmem_limit_bytes=VMEM_LIMIT),
    )(*args)


def place():
    frame = lax.axis_index("tm")
    return lax.axis_index("space"), lax.rem(frame, NEAR), lax.div(frame, NEAR)


def lane(shape):
    return lax.broadcasted_iota(jnp.int32, shape, len(shape) - 1)


def halves(x):
    hi = x.astype(BF)
    return hi, (x - hi.astype(F32)).astype(BF)


def joined(hi, lo):
    return hi.astype(F32) + lo.astype(F32)


def mm(a, b, dims):
    return lax.dot_general(a, b, (dims, ((), ())), preferred_element_type=F32)


NN = ((1,), (0,))
NT = ((1,), (1,))
TN = ((0,), (0,))


def flag(cond):
    return jnp.where(cond, 1.0, 0.0).astype(F32)


def pack(ref, mats):
    last = mats[7]
    lanes = lane((HD, LN))
    for i in range(7):
        piece = pltpu.roll(last, HD - 16 * i, 1) if i < 7 else last
        ref[HD * i : HD * (i + 1), :] = jnp.where(lanes < HD, mats[i], piece)
    ref[HD * 7 : HD * 8, :] = mats[8]
    ref[HD * 8 : HD * 9, :] = mats[9]
    ref[HD * 9 : ROWS, :] = jnp.zeros((ROWS - HD * 9, LN), F32)


def unpack(ref):
    lanes = lane((HD, LN))
    mats, last = [], jnp.zeros((HD, LN), F32)
    for i in range(7):
        x = ref[HD * i : HD * (i + 1), :]
        mats.append(jnp.where(lanes < HD, x, 0.0))
        inside = (lanes >= 16 * i) & (lanes < 16 * i + 16)
        last = jnp.where(inside, pltpu.roll(x, 16 + 16 * i, 1), last)
    return mats + [last, ref[HD * 7 : HD * 8, :], ref[HD * 8 : HD * 9, :]]


def pad_rows(x):
    return jnp.concatenate([x, jnp.zeros((LN - HD, LN), x.dtype)], axis=0)


def heads_of(tile):
    out = []
    for h in range(HEADS):
        t, off = divmod(HD * h, LN)
        x = tile(t)
        if off:
            x = pltpu.roll(x, LN - off, 1)
        if off + HD > LN:
            y = pltpu.roll(tile(t + 1), LN - off, 1)
            x = jnp.where(lane(x.shape) < LN - off, x, y)
        out.append(jnp.where(lane(x.shape) < HD, x, 0.0))
    return out


def tiles_of(heads):
    out = []
    for t in range(-(-HEADS * HD // LN)):
        first, off = divmod(LN * t, HD)
        x = heads[first]
        if off:
            x = pltpu.roll(x, LN - off, 1)
        left = HD - off
        while left < LN and first + 1 < HEADS:
            first += 1
            y = pltpu.roll(heads[first], left, 1)
            x = jnp.where(lane(x.shape) < left, x, y)
            left += HD
        out.append(x)
    return out


def loader(ref, rows, width):
    cache = {}

    def tile(t):
        if t not in cache:
            n = min(LN, width - LN * t)
            x = ref[0:rows, LN * t : LN * t + n].astype(F32)
            if n < LN:
                x = jnp.concatenate([x, jnp.zeros((rows, LN - n), F32)], axis=1)
            cache[t] = x
        return cache[t]

    return tile


def spread(refs, relu, keep, send):
    first = place()[0] == 0
    for j, ref in enumerate(refs):
        rows, width = ref.shape
        heads = heads_of(loader(ref, rows, width))
        for i in range(HC):
            a, b = heads[i], heads[i + HC]
            if relu[j]:
                a, b = jnp.maximum(a, 0.0), jnp.maximum(b, 0.0)
            keep[j, :, col(i)] = lax.select(first, a, b).astype(BF)
            send[j, :, col(i)] = lax.select(first, b, a).astype(BF)


def spread_k_kernel(k, keep, send):
    spread((k,), (True,), keep, send)


def spread_v_kernel(v, keep, send):
    spread((v,), (False,), keep, send)


def spread_qg_kernel(q, g, taps, after, keep, send, taps_out):
    first = place()[0] == 0
    spread((q, g), (True, False), keep, send)
    for a in range(3):
        heads = heads_of(loader(taps.at[a], 3, taps.shape[2]))
        for i in range(HC):
            taps_out[a, :, col(i)] = lax.select(first, heads[i], heads[i + HC])


def col(i):
    return slice(LN * i, LN * (i + 1))


def both(keep, recv, j, i):
    return jnp.concatenate([keep[j, :, col(i)], recv[j, :, col(i)]], axis=0)


def conv_kernel(keep_v, recv_v, keep_g, recv_g, taps, local, gc_mine, gc_other, taps_out):
    first = place()[0] == 0
    half = keep_v.shape[1]
    n = 2 * half
    cols = 32
    taps_out[...] = jnp.zeros_like(taps_out)
    pos = lax.broadcasted_iota(jnp.int32, (n, LN), 0) % cols
    zero_row = jnp.zeros((cols, LN), F32)

    def shifts(keep, recv, j, i):
        a, b = keep[j, :, col(i)].astype(F32), recv[j, :, col(i)].astype(F32)
        x = jnp.concatenate([lax.select(first, a, b), lax.select(first, b, a)], axis=0)
        before = jnp.where(pos == 0, 0.0, pltpu.roll(x, 1, 0))
        after = jnp.where(pos == cols - 1, 0.0, pltpu.roll(x, n - 1, 0))
        return before, x, after

    def up(u):
        return jnp.concatenate([zero_row, u[: n - cols]], axis=0)

    def down(u):
        return jnp.concatenate([u[cols:], zero_row], axis=0)

    def put(mine, other, x, i):
        mine[:, col(i)] = lax.select(first, x[:half], x[half:])
        other[:, col(i)] = lax.select(first, x[half:], x[:half])

    for i in range(HC):
        w = [taps[a, :, col(i)] for a in range(3)]
        vs, gs = shifts(keep_v, recv_v, 0, i), shifts(keep_g, recv_g, 1, i)
        u = [sum(w[a][b : b + 1] * vs[b] for b in range(3)) for a in range(3)]
        put(local.at[0:half], local.at[half:n], up(u[0]) + u[1] + down(u[2]), i)
        u = [sum(w[a][b : b + 1] * gs[2 - b] for b in range(3)) for a in range(3)]
        put(gc_mine, gc_other, down(u[0]) + u[1] + up(u[2]), i)
        g = gs[1]
        for b in range(3):
            s = vs[b]
            for a, prod in enumerate((g[cols:] * s[: n - cols], g * s, g[: n - cols] * s[cols:])):
                r = 9 * i + 3 * a + b
                taps_out[r // 24, r % 24 : r % 24 + 1, :] = jnp.sum(prod, axis=0, keepdims=True)


def rows_at(p, k, n):
    return pl.ds(pl.multiple_of((p ^ k) * n, n), n)


def put_rows(ref, *arrays):
    at = 0
    for x in arrays:
        ref[at : at + x.shape[0], :] = x
        at += x.shape[0]
    if at < ref.shape[0]:
        ref[at:, :] = jnp.zeros((ref.shape[0] - at, LN), F32)


def split(x):
    hi = x.astype(BF).astype(F32)
    return hi, x - hi


def vectors(block):
    x = block.astype(F32)
    return x[0:HC] + x[HC : 2 * HC], x[2 * HC : 3 * HC]


def partial_kernel(keep_k, recv_k, keep_v, recv_v, own, ksum, mean, a1, a2, a3, state, rows):
    p = place()[1]
    mats, sums, means = [], [], []
    for i in range(HC):
        keys, v = both(keep_k, recv_k, 0, i), both(keep_v, recv_v, 0, i).astype(F32)
        mid = (jnp.sum(v, axis=0, keepdims=True) * (1.0 / v.shape[0])).astype(BF).astype(F32)
        hi, lo = halves(v - mid)
        x = mm(keys, jnp.concatenate([hi, lo], axis=1), TN)[:HD]
        mats.append(x[:, :LN] + x[:, LN:])
        sums.append(jnp.sum(keys.astype(F32), axis=0, keepdims=True))
        means.append(mid)
    pack(state, mats)
    n = ROWS // NEAR
    own[...] = state[rows_at(p, 0, n), :]
    put_rows(ksum, *sums)
    put_rows(mean, *means)
    put_rows(rows, *split(ksum[0:HC, :]), mean[0:HC, :])
    block = rows[...].astype(BF)
    for k, ref in enumerate((a1, a2, a3), 1):
        ref[0:n, :] = state[rows_at(p, k, n), :].astype(BF)
        ref[n:, :] = block


def products(sums, means, i):
    free = jnp.zeros((-len(sums) % 8, LN), F32)
    a = jnp.concatenate([x[i : i + 1] for x in sums] + [free], axis=0)
    b = jnp.concatenate([x[i : i + 1] for x in means] + [free], axis=0)
    return lax.dot_general(
        a, b, (TN, ((), ())), precision=lax.Precision.HIGHEST, preferred_element_type=F32
    )[:HD]


def block_kernel(own, ksum, mean, a1, a2, a3, pay, kpre, state, rows):
    p = place()[1]
    n = ROWS // NEAR
    total, kp = own[...], ksum[0:HC, :]
    sums, means = [ksum[0:HC, :]], [mean[0:HC, :]]
    for k, ref in enumerate((a1, a2, a3), 1):
        total = total + ref[0:n, :].astype(F32)
        ks, mid = vectors(ref[n:, :])
        sums.append(ks)
        means.append(mid)
        kp = kp + flag((p ^ k) <= p) * ks
    kpre[...] = kp
    mid = (sum(means) * (1.0 / NEAR)).astype(BF).astype(F32)
    pack(state, [products(sums, [x - mid for x in means], i) for i in range(HC)])
    total = total + state[rows_at(p, 0, n), :]
    put_rows(rows, *split(sum(sums)), mid)
    block = rows[...].astype(BF)
    m = n // pay.shape[0]
    for b in range(pay.shape[0]):
        pay[b, 0:m, :] = total[m * b : m * (b + 1)].astype(BF)
        pay[b, m:, :] = block


def rank_kernel(got, ksum, mean, a1, a2, a3, rank):
    _, p, mine = place()
    n = ROWS // NEAR
    m = n // got.shape[0]
    sums, means = [ksum[0:HC, :]], [mean[0:HC, :]]
    for k, ref in enumerate((a1, a2, a3), 1):
        ks, mid = vectors(ref[n:, :])
        sums.append(flag((p ^ k) <= p) * ks)
        means.append(mid)
    for b in range(got.shape[0]):
        ks, mid = vectors(got[b, m:, :])
        sums.append(flag(b < mine) * ks)
        means.append(mid)
    for i in range(HC):
        rank[HD * i : HD * (i + 1), :] = products(sums, means, i)


def reciprocal_of(q, kt, i):
    row = jnp.broadcast_to(kt[i : i + 1, :], (LN, LN))
    hi, lo = halves(row)
    den = mm(jnp.concatenate([q, q], axis=1), jnp.concatenate([hi, lo], axis=1), NT)
    return 1.0 / (den + 1.0)


def turn_kernel(got, kpre, keep, recv, taps, down, kt, own, taps_own, c1, c2, c3, state, rows):
    _, p, mine = place()
    nb = got.shape[0]
    n = ROWS // NEAR
    m = n // nb
    run, key_total = jnp.zeros((m, LN), F32), kpre[...]
    for b in range(nb):
        down[b] = run.astype(BF)
        run = run + got[b, 0:m, :].astype(F32)
        ks, _ = vectors(got[b, m:, :])
        key_total = key_total + flag(b < mine) * ks
    kt[...] = key_total
    mats = []
    for i in range(HC):
        q = both(keep, recv, 0, i)
        scaled = both(keep, recv, 1, i).astype(F32) * reciprocal_of(q, key_total, i)
        hi, lo = halves(scaled)
        x = mm(q, jnp.concatenate([hi, lo], axis=1), TN)[:HD]
        mats.append(x[:, :LN] + x[:, LN:])
    pack(state, mats)
    own[...] = state[rows_at(p, 0, n), :]
    for k, ref in enumerate((c1, c2, c3), 1):
        ref[0:n, :] = state[rows_at(p, k, n), :].astype(BF)
        put_rows(rows, *split(taps[p ^ k]))
        ref[n:, :] = rows[...].astype(BF)
    taps_own[...] = taps[p]


def back_block_kernel(own, c1, c2, c3, down, taps, pay, rows):
    nb = pay.shape[0]
    n = ROWS // NEAR
    m = n // nb
    total, t = own[...], taps[...]
    for ref in (c1, c2, c3):
        total = total + ref[0:n, :].astype(F32)
        x = ref[n:, :].astype(F32)
        t = t + (x[0:24] + x[24:48])
    hi, lo = split(t)
    for b in range(nb):
        pay[b, 0:m, :] = down[b]
        pay[b, m : 2 * m, :] = total[m * b : m * (b + 1)].astype(BF)
        put_rows(rows, hi[3 * b : 3 * b + 3], lo[3 * b : 3 * b + 3])
        pay[b, 2 * m :, :] = rows[...].astype(BF)


def prefix_kernel(got, own, a1, a2, a3, s_own, e1, e2, e3, taps_own, back):
    p = place()[1]
    nb = got.shape[0]
    n = ROWS // NEAR
    m = n // nb
    base = jnp.concatenate([got[b, 0:m, :].astype(F32) for b in range(nb)], axis=0)
    run = jnp.zeros((m, LN), F32)
    t = jnp.zeros((3, LN), F32)
    for b in reversed(range(nb)):
        back[b] = run.astype(BF)
        run = run + got[b, m : 2 * m, :].astype(F32)
        x = got[b, 2 * m :, :].astype(F32)
        t = t + (x[0:3] + x[3:6])
    taps_own[...] = t
    parts = [own[...]] + [r[0:n, :].astype(F32) for r in (a1, a2, a3)]
    for k, ref in enumerate((s_own, e1, e2, e3)):
        x = base
        for j in range(NEAR):
            x = x + flag((p ^ j) <= (p ^ k)) * parts[j]
        ref[...] = x.astype(ref.dtype)


def attend_kernel(
    e1, e2, e3, s_own, rank, kt, keep, recv, local, taps_own, back, mine, other, pay, gks, state, rows
):
    p = place()[1]
    nb = pay.shape[0]
    n = ROWS // NEAR
    m = n // nb
    half = keep.shape[1]
    state[rows_at(p, 0, n), :] = s_own[...]
    taps = taps_own[...]
    for k, ref in enumerate((e1, e2, e3), 1):
        state[rows_at(p, k, n), :] = ref[...].astype(F32)
    mats = unpack(state)
    key_total = kt[...]
    ones = jnp.ones((2 * LN, LN), BF)
    for i in range(HC):
        q, g = both(keep, recv, 0, i), both(keep, recv, 1, i)
        hi, lo = halves(pad_rows(mats[i] + rank[HD * i : HD * (i + 1), :]))
        recip = reciprocal_of(q, key_total, i)
        out = mm(jnp.concatenate([q, q], axis=1), jnp.concatenate([hi, lo], axis=0), NN) * recip
        x = (out + local[:, col(i)]).astype(BF)
        mine[0, :, col(i)] = x[:half]
        other[0, :, col(i)] = x[half:]
        ghi, glo = halves(g.astype(F32) * out)
        gden = -mm(jnp.concatenate([ghi, glo], axis=1), ones, NN) * recip
        gs = mm(jnp.concatenate([g, g], axis=1), jnp.concatenate([hi, lo], axis=1), NT)
        qf = q.astype(F32)
        x = jnp.where(qf > 0.0, gs * recip + gden * key_total[i : i + 1, :], 0.0).astype(BF)
        mine[1, :, col(i)] = x[:half]
        other[1, :, col(i)] = x[half:]
        gks[i : i + 1, :] = jnp.sum(gden * qf, axis=0, keepdims=True)
    put_rows(rows, gks[...], *split(taps))
    block = rows[...].astype(BF)
    for b in range(nb):
        pay[b, 0:m, :] = back[b]
        pay[b, m:, :] = block


def suffix_kernel(got, own, c1, c2, c3, gks, after, g0, g1, g2, g3, rows):
    _, p, mine = place()
    nb = got.shape[0]
    n = ROWS // NEAR
    m = n // nb
    base = jnp.concatenate([got[b, 0:m, :].astype(F32) for b in range(nb)], axis=0)
    later = jnp.zeros((HC, LN), F32)
    taps = []
    for b in range(nb):
        x = got[b, m:, :].astype(F32)
        later = later + flag(b > mine) * x[0:HC]
        taps.append(x[HC : HC + 3] + x[HC + 3 : HC + 6])
    taps = jnp.concatenate(taps, axis=0)
    parts = [own[...]] + [r[0:n, :].astype(F32) for r in (c1, c2, c3)]
    for k, ref in enumerate((g0, g1, g2, g3)):
        x = base
        for j in range(NEAR):
            x = x + flag((p ^ j) >= (p ^ k)) * parts[j]
        ref[0:n, :] = x.astype(BF)
        put_rows(rows, later + flag(p >= (p ^ k)) * gks[...], jnp.zeros((HC, LN), F32), *split(taps))
        ref[n:, :] = rows[...].astype(BF)


def assembled(refs, state, taps):
    p = place()[1]
    n = ROWS // NEAR
    nb = taps.shape[0]
    total = jnp.zeros((HC, LN), F32)
    for k, ref in enumerate(refs):
        state[rows_at(p, k, n), :] = ref[0:n, :].astype(F32)
        x = ref[n:, :].astype(F32)
        total = total + x[0:HC]
        for b in range(nb):
            at = 2 * HC + 3 * b
            taps[b, p ^ k] = x[at : at + 3] + x[at + 3 * nb : at + 3 * nb + 3]
    return unpack(state), total


def key_value_grads(refs, tokens, conv, state, taps):
    mats, total = assembled(refs, state, taps)
    keys_out, values_out = [], []
    for i in range(HC):
        keys, v = tokens[0][0, :, col(i)], tokens[1][0, :, col(i)]
        hi, lo = halves(pad_rows(mats[i]))
        gk = mm(jnp.concatenate([v, v], axis=1), jnp.concatenate([hi, lo], axis=1), NT)
        keys_out.append(jnp.where(keys.astype(F32) > 0.0, gk + total[i : i + 1, :], 0.0))
        gm = mm(jnp.concatenate([keys, keys], axis=1), jnp.concatenate([hi, lo], axis=0), NN)
        values_out.append(gm + conv[:, col(i)])
    return keys_out, values_out


def half_kernel(g0, g1, g2, g3, keep_k, keep_v, gc_mine, side, taps, state):
    sides = key_value_grads((g0, g1, g2, g3), (keep_k, keep_v), gc_mine, state, taps)
    for j in range(2):
        for i in range(HC):
            side[j, :, col(i)] = sides[j][i].astype(BF)


def finish_kernel(o0, o1, o2, o3, send_k, send_v, gc_other, side, taps_a, key, value, taps, state, taps_b):
    first = place()[0] == 0
    sides = key_value_grads((o0, o1, o2, o3), (send_k, send_v), gc_other, state, taps_b)
    for j, ref in enumerate((key, value)):
        gather_heads(first, [side[j, :, col(i)].astype(F32) for i in range(HC)], sides[j], ref)
    for a in range(3):
        rows = []
        for scratch in (taps_a, taps_b):
            heads = []
            for i in range(HC):
                lines = []
                for b in range(3):
                    r = 9 * i + 3 * a + b
                    lines.append(scratch[(r % 24) // 3, r // 24, r % 3 : r % 3 + 1, :])
                heads.append(jnp.concatenate(lines, axis=0))
            rows.append(heads)
        gather_heads(first, rows[0], rows[1], taps.at[a])


def gather_heads(first, mine, other, ref):
    heads = [lax.select(first, mine[i], other[i]) for i in range(HC)]
    heads += [lax.select(first, other[i], mine[i]) for i in range(HC)]
    width = ref.shape[1]
    for t, x in enumerate(tiles_of(heads)):
        n = min(LN, width - LN * t)
        ref[:, LN * t : LN * t + n] = x[:, :n].astype(ref.dtype)


def merge_kernel(mine, other, out_a, out_b, done):
    done[...] = jnp.zeros_like(done)
    first = place()[0] == 0
    for j, ref in enumerate((out_a, out_b)):
        heads = [[x[j, :, col(i)].astype(F32) for i in range(HC)] for x in (mine, other)]
        gather_heads(first, heads[0], heads[1], ref)


def shards(query_pre, key_pre, value_pre, grad_out, conv_taps):
    shape = value_pre.shape
    width = shape[-1]
    t = shape[0] * shape[1] * shape[2]
    frames = lax.axis_size("tm")
    nb = frames // NEAR
    across = [[j + NEAR * b for b in range(nb)] for j in range(NEAR)]

    def over(x):
        return lax.ppermute(x, "space", [(0, 1), (1, 0)])

    def near(arrays):
        return [
            lax.ppermute(a, "tm", [(i, i ^ k) for i in range(frames)])
            for k, a in enumerate(arrays, 1)
        ]

    def far(x):
        return lax.all_to_all(x, "tm", 0, 0, axis_index_groups=across, tiled=True)

    n = ROWS // NEAR
    m = n // nb
    q, k, v, g = (x.reshape(t, width) for x in (query_pre, key_pre, value_pre, grad_out))
    pair = ((2, t, WC), BF)
    share = ((n, LN), F32)
    small = ((16, LN), F32)
    row = ((HC, LN), F32)
    state = ((ROWS, LN), F32)

    one = ((1, t, WC), BF)
    keep_k, send_k = call(spread_k_kernel, [one, one], k)
    recv_k = over(send_k)
    keep_v, send_v = call(spread_v_kernel, [one, one], v)
    recv_v = over(send_v)
    own_b, ksum, mean, *out = call(
        partial_kernel,
        [share, small, small] + [((n + 32, LN), BF)] * 3,
        keep_k, recv_k, keep_v, recv_v, scratch=[state, ((32, LN), F32)], us=1,
    )
    got_a = near(out)
    keep_qg, send_qg, taps = call(
        spread_qg_kernel, [pair, pair, ((3, 3, WC), F32)], q, g, conv_taps, ksum, us=1
    )
    recv_qg = over(send_qg)
    local, gc_mine, gc_other, taps_part = call(
        conv_kernel,
        [((2 * t, WC), F32), ((t, WC), F32), ((t, WC), F32), ((NEAR, 24, LN), F32)],
        keep_v, recv_v, keep_qg, recv_qg, taps, us=2,
    )
    gc_other = over(gc_other)
    pay, kpre = call(
        block_kernel,
        [((nb, m + 32, LN), BF), row],
        own_b, ksum, mean, *got_a, scratch=[state, ((32, LN), F32)],
    )
    got = far(pay)
    down, kt, own_d, taps_own, *out = call(
        turn_kernel,
        [((nb, m, LN), BF), row, share, ((24, LN), F32)] + [((n + 48, LN), BF)] * 3,
        got, kpre, keep_qg, recv_qg, taps_part, scratch=[state, ((48, LN), F32)], us=4,
    )
    got_c = near(out)
    (pay,) = call(
        back_block_kernel,
        [((nb, 2 * m + 8, LN), BF)],
        own_d, *got_c, down, taps_own, scratch=[((8, LN), F32)],
    )
    (rank,) = call(rank_kernel, [((HC * HD, LN), F32)], got, ksum, mean, *got_a, us=2)
    got = far(pay)
    s_own, e1, e2, e3, taps_own, back = call(
        prefix_kernel,
        [share] + [((n, LN), BF)] * 3 + [((3, LN), F32), ((nb, m, LN), BF)],
        got, own_b, *got_a,
    )
    got_e = near((e1, e2, e3))
    mine, other, pay, gks = call(
        attend_kernel,
        [pair, pair, ((nb, m + 16, LN), BF), row],
        *got_e, s_own, rank, kt, keep_qg, recv_qg, local, taps_own, back,
        scratch=[state, ((16, LN), F32)], us=4,
    )
    got = far(pay)
    whole = ((t, width), BF)
    attended, query_grad, done = call(
        merge_kernel, [whole, whole, ((8, LN), F32)], mine, over(other), us=2
    )
    tail = -(-(2 * HC + 6 * nb) // 8) * 8
    g0, *out = call(
        suffix_kernel,
        [((n + tail, LN), BF)] * 4,
        got, own_d, *got_c, gks, done, scratch=[((tail, LN), F32)],
    )
    gs = [g0] + near(out)
    quarters = ((nb, NEAR, 3, LN), F32)
    side, taps_mine = call(
        half_kernel, [pair, quarters], *gs, keep_k, keep_v, gc_mine, scratch=[state], us=2
    )
    key_grad, value_grad, taps_grad = call(
        finish_kernel,
        [whole, whole, (conv_taps.shape, F32)],
        *[over(x) for x in gs], send_k, send_v, gc_other, side, taps_mine,
        scratch=[state, quarters], us=2,
    )
    return (
        attended.reshape(shape),
        query_grad.reshape(shape),
        key_grad.reshape(shape),
        value_grad.reshape(shape),
        taps_grad,
    )


def solution(mesh):
    frame = P(("groups", "tm"), "space", None, None)
    return jax.shard_map(
        shards,
        mesh=mesh,
        in_specs=(frame, frame, frame, frame, P()),
        out_specs=(frame, frame, frame, frame, P("groups", None, None)),
        check_vma=False,
    )
```

```python
import functools

import jax
import jax.numpy as jnp
from jax import lax
from jax.experimental import pallas as pl
from jax.experimental.pallas import tpu as pltpu
from jax.sharding import PartitionSpec as P

HEADS = 20
HD = 112
LN = 128
HC = 10
WC = HC * LN
NEAR = 4
ROWS = 1024
F32 = jnp.float32
BF = jnp.bfloat16
INTERPRET = False
VMEM_LIMIT = 16 << 20


def call(kernel, outs, *args, scratch=(), us=1):
    return pl.pallas_call(
        kernel,
        out_shape=[jax.ShapeDtypeStruct(s, d) for s, d in outs],
        in_specs=[pl.BlockSpec(memory_space=pltpu.VMEM)] * len(args),
        out_specs=[pl.BlockSpec(memory_space=pltpu.VMEM)] * len(outs),
        scratch_shapes=[pltpu.VMEM(*s) if isinstance(s, tuple) else s for s in scratch],
        interpret=INTERPRET,
        cost_estimate=pl.CostEstimate(flops=us * 10**10, bytes_accessed=10**6, transcendentals=0),
        compiler_params=pltpu.CompilerParams(vmem_limit_bytes=VMEM_LIMIT),
    )(*args)


def place():
    frame = lax.axis_index("tm")
    return lax.axis_index("space"), lax.rem(frame, NEAR), lax.div(frame, NEAR)


def lane(shape):
    return lax.broadcasted_iota(jnp.int32, shape, len(shape) - 1)


def halves(x):
    hi = x.astype(BF)
    return hi, (x - hi.astype(F32)).astype(BF)


def joined(hi, lo):
    return hi.astype(F32) + lo.astype(F32)


def mm(a, b, dims):
    return lax.dot_general(a, b, (dims, ((), ())), preferred_element_type=F32)


NN = ((1,), (0,))
NT = ((1,), (1,))
TN = ((0,), (0,))


def flag(cond):
    return jnp.where(cond, 1.0, 0.0).astype(F32)


def pack(ref, mats):
    last = mats[7]
    lanes = lane((HD, LN))
    for i in range(7):
        piece = pltpu.roll(last, HD - 16 * i, 1) if i < 7 else last
        ref[HD * i : HD * (i + 1), :] = jnp.where(lanes < HD, mats[i], piece)
    ref[HD * 7 : HD * 8, :] = mats[8]
    ref[HD * 8 : HD * 9, :] = mats[9]
    ref[HD * 9 : ROWS, :] = jnp.zeros((ROWS - HD * 9, LN), F32)


def unpack(ref):
    lanes = lane((HD, LN))
    mats, last = [], jnp.zeros((HD, LN), F32)
    for i in range(7):
        x = ref[HD * i : HD * (i + 1), :]
        mats.append(jnp.where(lanes < HD, x, 0.0))
        inside = (lanes >= 16 * i) & (lanes < 16 * i + 16)
        last = jnp.where(inside, pltpu.roll(x, 16 + 16 * i, 1), last)
    return mats + [last, ref[HD * 7 : HD * 8, :], ref[HD * 8 : HD * 9, :]]


def pad_rows(x):
    return jnp.concatenate([x, jnp.zeros((LN - HD, LN), x.dtype)], axis=0)


def heads_of(tile):
    out = []
    for h in range(HEADS):
        t, off = divmod(HD * h, LN)
        x = tile(t)
        if off:
            x = pltpu.roll(x, LN - off, 1)
        if off + HD > LN:
            y = pltpu.roll(tile(t + 1), LN - off, 1)
            x = jnp.where(lane(x.shape) < LN - off, x, y)
        out.append(jnp.where(lane(x.shape) < HD, x, 0.0))
    return out


def tiles_of(heads):
    out = []
    for t in range(-(-HEADS * HD // LN)):
        first, off = divmod(LN * t, HD)
        x = heads[first]
        if off:
            x = pltpu.roll(x, LN - off, 1)
        left = HD - off
        while left < LN and first + 1 < HEADS:
            first += 1
            y = pltpu.roll(heads[first], left, 1)
            x = jnp.where(lane(x.shape) < left, x, y)
            left += HD
        out.append(x)
    return out


def loader(ref, rows, width):
    cache = {}

    def tile(t):
        if t not in cache:
            n = min(LN, width - LN * t)
            x = ref[0:rows, LN * t : LN * t + n].astype(F32)
            if n < LN:
                x = jnp.concatenate([x, jnp.zeros((rows, LN - n), F32)], axis=1)
            cache[t] = x
        return cache[t]

    return tile


def spread(refs, relu, keep, send):
    first = place()[0] == 0
    for j, ref in enumerate(refs):
        rows, width = ref.shape
        heads = heads_of(loader(ref, rows, width))
        for i in range(HC):
            a, b = heads[i], heads[i + HC]
            if relu[j]:
                a, b = jnp.maximum(a, 0.0), jnp.maximum(b, 0.0)
            keep[j, :, col(i)] = lax.select(first, a, b).astype(BF)
            send[j, :, col(i)] = lax.select(first, b, a).astype(BF)


def spread_k_kernel(k, keep, send):
    spread((k,), (True,), keep, send)


def spread_v_kernel(v, keep, send):
    spread((v,), (False,), keep, send)


def spread_qg_kernel(q, g, taps, after, keep, send, taps_out):
    first = place()[0] == 0
    spread((q, g), (True, False), keep, send)
    for a in range(3):
        heads = heads_of(loader(taps.at[a], 3, taps.shape[2]))
        for i in range(HC):
            taps_out[a, :, col(i)] = lax.select(first, heads[i], heads[i + HC])


def col(i):
    return slice(LN * i, LN * (i + 1))


def both(keep, recv, j, i):
    return jnp.concatenate([keep[j, :, col(i)], recv[j, :, col(i)]], axis=0)


def conv_kernel(keep_v, recv_v, keep_g, recv_g, taps, local, gc_mine, gc_other, taps_out):
    first = place()[0] == 0
    half = keep_v.shape[1]
    n = 2 * half
    cols = 32
    taps_out[...] = jnp.zeros_like(taps_out)
    pos = lax.broadcasted_iota(jnp.int32, (n, LN), 0) % cols
    zero_row = jnp.zeros((cols, LN), F32)

    def shifts(keep, recv, j, i):
        a, b = keep[j, :, col(i)].astype(F32), recv[j, :, col(i)].astype(F32)
        x = jnp.concatenate([lax.select(first, a, b), lax.select(first, b, a)], axis=0)
        before = jnp.where(pos == 0, 0.0, pltpu.roll(x, 1, 0))
        after = jnp.where(pos == cols - 1, 0.0, pltpu.roll(x, n - 1, 0))
        return before, x, after

    def up(u):
        return jnp.concatenate([zero_row, u[: n - cols]], axis=0)

    def down(u):
        return jnp.concatenate([u[cols:], zero_row], axis=0)

    def put(mine, other, x, i):
        mine[:, col(i)] = lax.select(first, x[:half], x[half:])
        other[:, col(i)] = lax.select(first, x[half:], x[:half])

    for i in range(HC):
        w = [taps[a, :, col(i)] for a in range(3)]
        vs, gs = shifts(keep_v, recv_v, 0, i), shifts(keep_g, recv_g, 1, i)
        u = [sum(w[a][b : b + 1] * vs[b] for b in range(3)) for a in range(3)]
        put(local.at[0:half], local.at[half:n], up(u[0]) + u[1] + down(u[2]), i)
        u = [sum(w[a][b : b + 1] * gs[2 - b] for b in range(3)) for a in range(3)]
        put(gc_mine, gc_other, down(u[0]) + u[1] + up(u[2]), i)
        g = gs[1]
        for b in range(3):
            s = vs[b]
            for a, prod in enumerate((g[cols:] * s[: n - cols], g * s, g[: n - cols] * s[cols:])):
                r = 9 * i + 3 * a + b
                taps_out[r // 24, r % 24 : r % 24 + 1, :] = jnp.sum(prod, axis=0, keepdims=True)


def rows_at(p, k, n):
    return pl.ds(pl.multiple_of((p ^ k) * n, n), n)


def put_rows(ref, *arrays):
    at = 0
    for x in arrays:
        ref[at : at + x.shape[0], :] = x
        at += x.shape[0]
    if at < ref.shape[0]:
        ref[at:, :] = jnp.zeros((ref.shape[0] - at, LN), F32)


def split(x):
    hi = x.astype(BF).astype(F32)
    return hi, x - hi


def vectors(block):
    x = block.astype(F32)
    return x[0:HC] + x[HC : 2 * HC], x[2 * HC : 3 * HC]


def partial_kernel(keep_k, recv_k, keep_v, recv_v, own, ksum, mean, a1, a2, a3, state, rows):
    p = place()[1]
    mats, sums, means = [], [], []
    for i in range(HC):
        keys, v = both(keep_k, recv_k, 0, i), both(keep_v, recv_v, 0, i).astype(F32)
        mid = (jnp.sum(v, axis=0, keepdims=True) * (1.0 / v.shape[0])).astype(BF).astype(F32)
        hi, lo = halves(v - mid)
        x = mm(keys, jnp.concatenate([hi, lo], axis=1), TN)[:HD]
        mats.append(x[:, :LN] + x[:, LN:])
        sums.append(jnp.sum(keys.astype(F32), axis=0, keepdims=True))
        means.append(mid)
    pack(state, mats)
    n = ROWS // NEAR
    own[...] = state[rows_at(p, 0, n), :]
    put_rows(ksum, *sums)
    put_rows(mean, *means)
    put_rows(rows, *split(ksum[0:HC, :]), mean[0:HC, :])
    block = rows[...].astype(BF)
    for k, ref in enumerate((a1, a2, a3), 1):
        ref[0:n, :] = state[rows_at(p, k, n), :].astype(BF)
        ref[n:, :] = block


def products(sums, means, i):
    free = jnp.zeros((-len(sums) % 8, LN), F32)
    a = jnp.concatenate([x[i : i + 1] for x in sums] + [free], axis=0)
    b = jnp.concatenate([x[i : i + 1] for x in means] + [free], axis=0)
    return lax.dot_general(
        a, b, (TN, ((), ())), precision=lax.Precision.HIGHEST, preferred_element_type=F32
    )[:HD]


def block_kernel(own, ksum, mean, a1, a2, a3, pay, kpre, state, rows):
    p = place()[1]
    n = ROWS // NEAR
    total, kp = own[...], ksum[0:HC, :]
    sums, means = [ksum[0:HC, :]], [mean[0:HC, :]]
    for k, ref in enumerate((a1, a2, a3), 1):
        total = total + ref[0:n, :].astype(F32)
        ks, mid = vectors(ref[n:, :])
        sums.append(ks)
        means.append(mid)
        kp = kp + flag((p ^ k) <= p) * ks
    kpre[...] = kp
    mid = (sum(means) * (1.0 / NEAR)).astype(BF).astype(F32)
    pack(state, [products(sums, [x - mid for x in means], i) for i in range(HC)])
    total = total + state[rows_at(p, 0, n), :]
    put_rows(rows, *split(sum(sums)), mid)
    block = rows[...].astype(BF)
    m = n // pay.shape[0]
    for b in range(pay.shape[0]):
        pay[b, 0:m, :] = total[m * b : m * (b + 1)].astype(BF)
        pay[b, m:, :] = block


def rank_kernel(got, ksum, mean, a1, a2, a3, kt, keep, recv, rank, recip):
    _, p, mine = place()
    n = ROWS // NEAR
    m = n // got.shape[0]
    sums, means = [ksum[0:HC, :]], [mean[0:HC, :]]
    for k, ref in enumerate((a1, a2, a3), 1):
        ks, mid = vectors(ref[n:, :])
        sums.append(flag((p ^ k) <= p) * ks)
        means.append(mid)
    for b in range(got.shape[0]):
        ks, mid = vectors(got[b, m:, :])
        sums.append(flag(b < mine) * ks)
        means.append(mid)
    for i in range(HC):
        rank[HD * i : HD * (i + 1), :] = products(sums, means, i)
        recip[:, col(i)] = reciprocal_of(both(keep, recv, 0, i), kt, i)


def reciprocal_of(q, kt, i):
    row = jnp.broadcast_to(kt[i : i + 1, :], (LN, LN))
    hi, lo = halves(row)
    den = mm(jnp.concatenate([q, q], axis=1), jnp.concatenate([hi, lo], axis=1), NT)
    return 1.0 / (den + 1.0)


def turn_kernel(got, kpre, keep, recv, taps, down, kt, own, taps_own, c1, c2, c3, state, rows):
    _, p, mine = place()
    nb = got.shape[0]
    n = ROWS // NEAR
    m = n // nb
    run, key_total = jnp.zeros((m, LN), F32), kpre[...]
    for b in range(nb):
        down[b] = run.astype(BF)
        run = run + got[b, 0:m, :].astype(F32)
        ks, _ = vectors(got[b, m:, :])
        key_total = key_total + flag(b < mine) * ks
    kt[...] = key_total
    mats = []
    for i in range(HC):
        q = both(keep, recv, 0, i)
        scaled = both(keep, recv, 1, i).astype(F32) * reciprocal_of(q, key_total, i)
        hi, lo = halves(scaled)
        x = mm(q, jnp.concatenate([hi, lo], axis=1), TN)[:HD]
        mats.append(x[:, :LN] + x[:, LN:])
    pack(state, mats)
    own[...] = state[rows_at(p, 0, n), :]
    for k, ref in enumerate((c1, c2, c3), 1):
        ref[0:n, :] = state[rows_at(p, k, n), :].astype(BF)
        put_rows(rows, *split(taps[p ^ k]))
        ref[n:, :] = rows[...].astype(BF)
    taps_own[...] = taps[p]


def back_block_kernel(own, c1, c2, c3, down, taps, pay, rows):
    nb = pay.shape[0]
    n = ROWS // NEAR
    m = n // nb
    total, t = own[...], taps[...]
    for ref in (c1, c2, c3):
        total = total + ref[0:n, :].astype(F32)
        x = ref[n:, :].astype(F32)
        t = t + (x[0:24] + x[24:48])
    hi, lo = split(t)
    for b in range(nb):
        pay[b, 0:m, :] = down[b]
        pay[b, m : 2 * m, :] = total[m * b : m * (b + 1)].astype(BF)
        put_rows(rows, hi[3 * b : 3 * b + 3], lo[3 * b : 3 * b + 3])
        pay[b, 2 * m :, :] = rows[...].astype(BF)


def prefix_kernel(got, own, a1, a2, a3, s_own, e1, e2, e3, taps_own, back):
    p = place()[1]
    nb = got.shape[0]
    n = ROWS // NEAR
    m = n // nb
    base = jnp.concatenate([got[b, 0:m, :].astype(F32) for b in range(nb)], axis=0)
    run = jnp.zeros((m, LN), F32)
    t = jnp.zeros((3, LN), F32)
    for b in reversed(range(nb)):
        back[b] = run.astype(BF)
        run = run + got[b, m : 2 * m, :].astype(F32)
        x = got[b, 2 * m :, :].astype(F32)
        t = t + (x[0:3] + x[3:6])
    taps_own[...] = t
    parts = [own[...]] + [r[0:n, :].astype(F32) for r in (a1, a2, a3)]
    for k, ref in enumerate((s_own, e1, e2, e3)):
        x = base
        for j in range(NEAR):
            x = x + flag((p ^ j) <= (p ^ k)) * parts[j]
        ref[...] = x.astype(ref.dtype)


def attend_kernel(
    e1, e2, e3, s_own, rank, recips, kt, keep, recv, local, taps_own, back, mine, other, pay, gks, state, rows
):
    p = place()[1]
    nb = pay.shape[0]
    n = ROWS // NEAR
    m = n // nb
    half = keep.shape[1]
    state[rows_at(p, 0, n), :] = s_own[...]
    taps = taps_own[...]
    for k, ref in enumerate((e1, e2, e3), 1):
        state[rows_at(p, k, n), :] = ref[...].astype(F32)
    mats = unpack(state)
    key_total = kt[...]
    ones = jnp.ones((2 * LN, LN), BF)
    for i in range(HC):
        q, g = both(keep, recv, 0, i), both(keep, recv, 1, i)
        hi, lo = halves(pad_rows(mats[i] + rank[HD * i : HD * (i + 1), :]))
        recip = recips[:, col(i)]
        out = mm(jnp.concatenate([q, q], axis=1), jnp.concatenate([hi, lo], axis=0), NN) * recip
        x = (out + local[:, col(i)]).astype(BF)
        mine[0, :, col(i)] = x[:half]
        other[0, :, col(i)] = x[half:]
        ghi, glo = halves(g.astype(F32) * out)
        gden = -mm(jnp.concatenate([ghi, glo], axis=1), ones, NN) * recip
        gs = mm(jnp.concatenate([g, g], axis=1), jnp.concatenate([hi, lo], axis=1), NT)
        qf = q.astype(F32)
        x = jnp.where(qf > 0.0, gs * recip + gden * key_total[i : i + 1, :], 0.0).astype(BF)
        mine[1, :, col(i)] = x[:half]
        other[1, :, col(i)] = x[half:]
        gks[i : i + 1, :] = jnp.sum(gden * qf, axis=0, keepdims=True)
    put_rows(rows, gks[...], *split(taps))
    block = rows[...].astype(BF)
    for b in range(nb):
        pay[b, 0:m, :] = back[b]
        pay[b, m:, :] = block


def suffix_kernel(got, own, c1, c2, c3, gks, after, g0, g1, g2, g3, rows):
    _, p, mine = place()
    nb = got.shape[0]
    n = ROWS // NEAR
    m = n // nb
    base = jnp.concatenate([got[b, 0:m, :].astype(F32) for b in range(nb)], axis=0)
    later = jnp.zeros((HC, LN), F32)
    taps = []
    for b in range(nb):
        x = got[b, m:, :].astype(F32)
        later = later + flag(b > mine) * x[0:HC]
        taps.append(x[HC : HC + 3] + x[HC + 3 : HC + 6])
    taps = jnp.concatenate(taps, axis=0)
    parts = [own[...]] + [r[0:n, :].astype(F32) for r in (c1, c2, c3)]
    for k, ref in enumerate((g0, g1, g2, g3)):
        x = base
        for j in range(NEAR):
            x = x + flag((p ^ j) >= (p ^ k)) * parts[j]
        ref[0:n, :] = x.astype(BF)
        put_rows(rows, later + flag(p >= (p ^ k)) * gks[...], jnp.zeros((HC, LN), F32), *split(taps))
        ref[n:, :] = rows[...].astype(BF)


def assembled(refs, state, taps):
    p = place()[1]
    n = ROWS // NEAR
    nb = taps.shape[0]
    total = jnp.zeros((HC, LN), F32)
    for k, ref in enumerate(refs):
        state[rows_at(p, k, n), :] = ref[0:n, :].astype(F32)
        x = ref[n:, :].astype(F32)
        total = total + x[0:HC]
        for b in range(nb):
            at = 2 * HC + 3 * b
            taps[b, p ^ k] = x[at : at + 3] + x[at + 3 * nb : at + 3 * nb + 3]
    return unpack(state), total


def key_value_grads(refs, tokens, conv, state, taps):
    mats, total = assembled(refs, state, taps)
    keys_out, values_out = [], []
    for i in range(HC):
        keys, v = tokens[0][0, :, col(i)], tokens[1][0, :, col(i)]
        hi, lo = halves(pad_rows(mats[i]))
        gk = mm(jnp.concatenate([v, v], axis=1), jnp.concatenate([hi, lo], axis=1), NT)
        keys_out.append(jnp.where(keys.astype(F32) > 0.0, gk + total[i : i + 1, :], 0.0))
        gm = mm(jnp.concatenate([keys, keys], axis=1), jnp.concatenate([hi, lo], axis=0), NN)
        values_out.append(gm + conv[:, col(i)])
    return keys_out, values_out


def half_kernel(g0, g1, g2, g3, keep_k, keep_v, gc_mine, side, taps, state):
    sides = key_value_grads((g0, g1, g2, g3), (keep_k, keep_v), gc_mine, state, taps)
    for j in range(2):
        for i in range(HC):
            side[j, :, col(i)] = sides[j][i].astype(BF)


def finish_kernel(o0, o1, o2, o3, send_k, send_v, gc_other, side, taps_a, key, value, taps, state, taps_b):
    first = place()[0] == 0
    sides = key_value_grads((o0, o1, o2, o3), (send_k, send_v), gc_other, state, taps_b)
    for j, ref in enumerate((key, value)):
        gather_heads(first, [side[j, :, col(i)].astype(F32) for i in range(HC)], sides[j], ref)
    for a in range(3):
        rows = []
        for scratch in (taps_a, taps_b):
            heads = []
            for i in range(HC):
                lines = []
                for b in range(3):
                    r = 9 * i + 3 * a + b
                    lines.append(scratch[(r % 24) // 3, r // 24, r % 3 : r % 3 + 1, :])
                heads.append(jnp.concatenate(lines, axis=0))
            rows.append(heads)
        gather_heads(first, rows[0], rows[1], taps.at[a])


def gather_heads(first, mine, other, ref):
    heads = [lax.select(first, mine[i], other[i]) for i in range(HC)]
    heads += [lax.select(first, other[i], mine[i]) for i in range(HC)]
    width = ref.shape[1]
    for t, x in enumerate(tiles_of(heads)):
        n = min(LN, width - LN * t)
        ref[:, LN * t : LN * t + n] = x[:, :n].astype(ref.dtype)


def merge_kernel(mine, other, out_a, out_b, done):
    done[...] = jnp.zeros_like(done)
    first = place()[0] == 0
    for j, ref in enumerate((out_a, out_b)):
        heads = [[x[j, :, col(i)].astype(F32) for i in range(HC)] for x in (mine, other)]
        gather_heads(first, heads[0], heads[1], ref)


def shards(query_pre, key_pre, value_pre, grad_out, conv_taps):
    shape = value_pre.shape
    width = shape[-1]
    t = shape[0] * shape[1] * shape[2]
    frames = lax.axis_size("tm")
    nb = frames // NEAR
    across = [[j + NEAR * b for b in range(nb)] for j in range(NEAR)]

    def over(x):
        return lax.ppermute(x, "space", [(0, 1), (1, 0)])

    def near(arrays):
        return [
            lax.ppermute(a, "tm", [(i, i ^ k) for i in range(frames)])
            for k, a in enumerate(arrays, 1)
        ]

    def far(x):
        return lax.all_to_all(x, "tm", 0, 0, axis_index_groups=across, tiled=True)

    n = ROWS // NEAR
    m = n // nb
    q, k, v, g = (x.reshape(t, width) for x in (query_pre, key_pre, value_pre, grad_out))
    pair = ((2, t, WC), BF)
    share = ((n, LN), F32)
    small = ((16, LN), F32)
    row = ((HC, LN), F32)
    state = ((ROWS, LN), F32)

    one = ((1, t, WC), BF)
    keep_k, send_k = call(spread_k_kernel, [one, one], k)
    recv_k = over(send_k)
    keep_v, send_v = call(spread_v_kernel, [one, one], v)
    recv_v = over(send_v)
    own_b, ksum, mean, *out = call(
        partial_kernel,
        [share, small, small] + [((n + 32, LN), BF)] * 3,
        keep_k, recv_k, keep_v, recv_v, scratch=[state, ((32, LN), F32)], us=1,
    )
    got_a = near(out)
    keep_qg, send_qg, taps = call(
        spread_qg_kernel, [pair, pair, ((3, 3, WC), F32)], q, g, conv_taps, ksum, us=1
    )
    recv_qg = over(send_qg)
    local, gc_mine, gc_other, taps_part = call(
        conv_kernel,
        [((2 * t, WC), F32), ((t, WC), F32), ((t, WC), F32), ((NEAR, 24, LN), F32)],
        keep_v, recv_v, keep_qg, recv_qg, taps, us=2,
    )
    gc_other = over(gc_other)
    pay, kpre = call(
        block_kernel,
        [((nb, m + 32, LN), BF), row],
        own_b, ksum, mean, *got_a, scratch=[state, ((32, LN), F32)],
    )
    got = far(pay)
    down, kt, own_d, taps_own, *out = call(
        turn_kernel,
        [((nb, m, LN), BF), row, share, ((24, LN), F32)] + [((n + 48, LN), BF)] * 3,
        got, kpre, keep_qg, recv_qg, taps_part, scratch=[state, ((48, LN), F32)], us=4,
    )
    got_c = near(out)
    (pay,) = call(
        back_block_kernel,
        [((nb, 2 * m + 8, LN), BF)],
        own_d, *got_c, down, taps_own, scratch=[((8, LN), F32)],
    )
    rank, recip = call(
        rank_kernel,
        [((HC * HD, LN), F32), ((2 * t, WC), F32)],
        got, ksum, mean, *got_a, kt, keep_qg, recv_qg, us=2,
    )
    got = far(pay)
    s_own, e1, e2, e3, taps_own, back = call(
        prefix_kernel,
        [share] + [((n, LN), BF)] * 3 + [((3, LN), F32), ((nb, m, LN), BF)],
        got, own_b, *got_a,
    )
    got_e = near((e1, e2, e3))
    mine, other, pay, gks = call(
        attend_kernel,
        [pair, pair, ((nb, m + 16, LN), BF), row],
        *got_e, s_own, rank, recip, kt, keep_qg, recv_qg, local, taps_own, back,
        scratch=[state, ((16, LN), F32)], us=4,
    )
    got = far(pay)
    whole = ((t, width), BF)
    attended, query_grad, done = call(
        merge_kernel, [whole, whole, ((8, LN), F32)], mine, over(other), us=2
    )
    tail = -(-(2 * HC + 6 * nb) // 8) * 8
    g0, *out = call(
        suffix_kernel,
        [((n + tail, LN), BF)] * 4,
        got, own_d, *got_c, gks, done, scratch=[((tail, LN), F32)],
    )
    gs = [g0] + near(out)
    quarters = ((nb, NEAR, 3, LN), F32)
    side, taps_mine = call(
        half_kernel, [pair, quarters], *gs, keep_k, keep_v, gc_mine, scratch=[state], us=2
    )
    key_grad, value_grad, taps_grad = call(
        finish_kernel,
        [whole, whole, (conv_taps.shape, F32)],
        *[over(x) for x in gs], send_k, send_v, gc_other, side, taps_mine,
        scratch=[state, quarters], us=2,
    )
    return (
        attended.reshape(shape),
        query_grad.reshape(shape),
        key_grad.reshape(shape),
        value_grad.reshape(shape),
        taps_grad,
    )


def solution(mesh):
    frame = P(("groups", "tm"), "space", None, None)
    return jax.shard_map(
        shards,
        mesh=mesh,
        in_specs=(frame, frame, frame, frame, P()),
        out_specs=(frame, frame, frame, frame, P("groups", None, None)),
        check_vma=False,
    )
```
